32 devices in a mesh: expert: 8 (over y, x, core), row: 4 (over z).
Axes of the slice: x: 2, y: 2, z: 4, core: 2. Of those that a mesh axis runs over, the one named last changes fastest.
Arguments:
- weights: bfloat16 [8, 7168, 2048], P('expert', 'row'), may hold values from -6 to 6
- left_bits: int32 [8, 7168], P('expert', 'row'), may hold values from 0 to 1
- right_bits: int32 [8, 2048], P('expert'), may hold values from 0 to 1
- groups: int32 [8, 2048], P('expert'), may hold values from 0 to 15, never falling along the last dimension, each value on 1 to 256 neighbouring positions
Outputs:
- scaled: bfloat16 [8, 7168, 2048], P('expert', 'row')
- block_error: float32 [8, 7168, 256], P('expert', 'row')
- scales: float32 [8, 16], P('expert')
- expert_error: float32 [8], P('expert')
- total_error: float32 [], replicated
The draws below stay inside these ranges and needn't reach their ends.
Inputs may be any that keep to these rules, and one draw needn't show every extreme that they name: Along each expert's 2048 columns the group number never falls; each of the 16 groups holds 1 to 256 columns.
All inputs are finite; a program needn't handle non-finite values.
Results may differ from the reference program's by a relative error of at most 0.0091.
Values may be sent and summed in bfloat16 or wider, within the bound.
A program may use at most 192 MiB of HBM per device.

```python
import math
import jax
import jax.numpy as jnp
import numpy as np
from jax import lax

D = 7168
FF = 2048
HB = 128
OUTER = 16
GROUPS = 16
BLOCKS = 56
GROUP_MOST = 256
EXPERTS = 8


def draw_weights(key, part):
    scale_key = jax.random.fold_in(key, 11)
    entry_key = jax.random.fold_in(key, 12)
    magnitude = jnp.exp(jax.random.uniform(scale_key, (EXPERTS, 1, 1), jnp.float32, math.log(0.02), math.log(1.0)))
    entries = jnp.clip(jax.random.normal(entry_key, (EXPERTS, D, FF), jnp.float32), -6.0, 6.0)
    return jnp.clip(entries * magnitude, -6.0, 6.0).astype(jnp.bfloat16)


def place_ends(result, stream_key, low, high):
    longest = result.shape.index(max(result.shape))
    spots = []
    for shift in (0, 1):
        where = [jax.random.randint(jax.random.fold_in(stream_key, axis), (), 0, length) for axis, length in enumerate(result.shape)]
        where[longest] = (where[longest] + shift) % result.shape[longest]
        spots.append(tuple(where))
    return result.at[spots[0]].set(low).at[spots[1]].set(high)


def profile(number_of, total, most, slope):
    loads = [(1 << 20) // math.isqrt(grade ** slope) + 1 for grade in range(2, number_of + 1)]
    spare, holding = total - most - (number_of - 1), [1] * (number_of - 1)
    while spare > 0:
        free = [i for i in range(number_of - 1) if holding[i] < most]
        whole, left = sum([loads[i] for i in free]), spare
        for i in free:
            more = min(most - holding[i], max(1, left * loads[i] // whole), spare)
            holding[i] = holding[i] + more
            spare = spare - more
    return np.array([most] + holding)


def ragged(key, amount, total, bound, skew):
    if amount == 2:
        one = jax.random.randint(key, (), max(1, total - bound), min(bound, total - 1) + 1)
        return jnp.stack([one, total - one])
    lengths = jnp.asarray(profile(amount, total, bound, skew), jnp.int32)
    couples = (amount - 1) // 2
    donor, receiver = lengths[1:1 + 2 * couples:2], lengths[2:2 + 2 * couples:2]
    room = jnp.minimum(donor - 1, bound - receiver)
    passed = jax.random.randint(jax.random.fold_in(key, 1), (couples,), 0, 1 << 20) % (room + 1)
    lengths = lengths.at[1:1 + 2 * couples:2].set(donor - passed).at[2:2 + 2 * couples:2].set(receiver + passed)
    return lengths[jax.random.permutation(jax.random.fold_in(key, 2), amount)]


def setup_inputs(seed: int = 0) -> dict:
    streams_of = jax.random.split(jax.random.key(seed), 5)
    return {
        "weights": draw_weights(jax.random.fold_in(streams_of[4], 71), 0),
        "left_bits": place_ends(jax.random.randint(streams_of[1], (EXPERTS, D), 0, 2), jax.random.fold_in(streams_of[1], 1), 0, 1).astype(jnp.int32),
        "right_bits": place_ends(jax.random.randint(streams_of[2], (EXPERTS, FF), 0, 2), jax.random.fold_in(streams_of[2], 1), 0, 1).astype(jnp.int32),
        "groups": jax.vmap(lambda own: jnp.searchsorted(jnp.cumsum(ragged(own, GROUPS, FF, GROUP_MOST, 1)), jnp.arange(FF), side="right"))(jax.random.split(streams_of[3], EXPERTS)).reshape((EXPERTS, FF)).astype(jnp.int32),
    }


def sylvester(order):
    row_index = jnp.arange(order, dtype=jnp.int32)[:, None]
    col_index = jnp.arange(order, dtype=jnp.int32)[None, :]
    common = jnp.bitwise_and(row_index, col_index)
    parity = jnp.zeros((order, order), jnp.int32)
    for bit_pos in range(order.bit_length() - 1):
        parity = parity + jnp.bitwise_and(jnp.right_shift(common, bit_pos), 1)
    return (1 - 2 * jnp.bitwise_and(parity, 1)).astype(jnp.float32)

def cosine_block(order):
    first = jnp.arange(order, dtype=jnp.float32)[:, None]
    second = jnp.arange(order, dtype=jnp.float32)[None, :]
    table = math.sqrt(2.0 / order) * jnp.cos(math.pi * (2.0 * second + 1.0) * first / (2.0 * order))
    return jnp.where(first == 0.0, table * math.sqrt(0.5), table)

def coset_error(values):
    nearest = jnp.floor(values + 0.5)
    offset = values - nearest
    squares = lax.optimization_barrier(jnp.sum(offset * offset, axis=-1))
    largest = lax.optimization_barrier(jnp.max(jnp.abs(offset), axis=-1))
    parity = jnp.mod(lax.optimization_barrier(jnp.sum(nearest, axis=-1)), 2.0)
    return jnp.where(parity > 0.5, squares + 1.0 - 2.0 * largest, squares)

def lattice_error(values):
    octets = values.reshape(values.shape[:-1] + (values.shape[-1] // 8, 8))
    return jnp.minimum(coset_error(octets), coset_error(octets - 0.5))

def reference(weights, left_bits, right_bits, groups):
    column_hadamard = sylvester(FF // OUTER)
    outer_hadamard = sylvester(OUTER)
    row_hadamard = sylvester(HB)
    block_matrix = cosine_block(BLOCKS).astype(jnp.bfloat16).astype(jnp.float32)
    group_ids = jnp.arange(GROUPS, dtype=jnp.int32)
    row_weight = (1.0 + 4.0 * (jnp.arange(D, dtype=jnp.float32) + 0.5) / D) / 3.0
    high = lax.Precision.HIGHEST

    def one_expert(operands):
        weight, left, right, group = operands
        left_sign = (2 * left - 1).astype(jnp.float32)
        right_sign = (2 * right - 1).astype(jnp.float32)
        signed = (weight.astype(jnp.float32) * left_sign[:, None] * right_sign[None, :]).astype(jnp.bfloat16)
        shaped = signed.astype(jnp.float32).reshape(D, OUTER, FF // OUTER)
        inner = jnp.einsum('dpq,qs->dps', shaped, column_hadamard, precision=high)
        outer = jnp.einsum('dps,pt->dts', inner, outer_hadamard, precision=high)
        columns = (outer.reshape(D, FF) / math.sqrt(FF)).astype(jnp.bfloat16)
        blocked = columns.astype(jnp.float32).reshape(BLOCKS, HB, FF)
        mixed_rows = jnp.einsum('ij,jbf->ibf', block_matrix, blocked, precision=high)
        rotated = jnp.einsum('ibf,bk->ikf', mixed_rows, row_hadamard, precision=high) / math.sqrt(HB)
        rotated = rotated.reshape(D, FF)
        column_peak = lax.optimization_barrier(jnp.max(jnp.abs(rotated), axis=0))
        in_group = group[None, :] == group_ids[:, None]
        group_peak = jnp.maximum(lax.optimization_barrier(jnp.max(jnp.where(in_group, column_peak[None, :], 0.0), axis=1)), 1.0)
        column_scale = lax.optimization_barrier(jnp.sum(jnp.where(in_group, (2.0 / group_peak)[:, None], 0.0), axis=0))
        values = rotated * column_scale[None, :]
        block_errors = lattice_error(values)
        mean_error = jnp.sum(block_errors * row_weight[:, None]) / (D * FF // 8)
        return (values.astype(jnp.bfloat16), block_errors, group_peak / 2.0, mean_error)
    scaled, block_error, scales, expert_error = lax.map(one_expert, (weights, left_bits, right_bits, groups))
    total_error = jnp.mean(expert_error)
    return (scaled, block_error, scales, expert_error, total_error)
```

```python
import functools
import math

import jax
import jax.numpy as jnp
import numpy as np
from jax import lax
from jax.experimental import pallas as pl
from jax.experimental.pallas import tpu as pltpu
from jax.sharding import PartitionSpec as P

HB = 128
SUB = 16
FOLD = HB // SUB
OCT = 8
LANES = 128
GROUPS = 16
BLOCKS = 56
SLAB = 256
PACK = LANES * OCT // SLAB
MESH = pl.DeviceIdType.MESH


def signs(common, bits):
    for shift in (4, 2, 1):
        if shift < bits:
            common = common ^ (common >> shift)
    return (1 - 2 * (common & 1)).astype(jnp.float32)


def iota(shape, dim):
    return lax.broadcasted_iota(jnp.int32, shape, dim)


def down(row):
    return jnp.broadcast_to(row, (LANES, LANES)).T


def cosine_table(order):
    first = np.arange(order, dtype=np.float64)[:, None]
    second = np.arange(order, dtype=np.float64)[None, :]
    table = math.sqrt(2.0 / order) * np.cos(math.pi * (2.0 * second + 1.0) * first / (2.0 * order))
    return np.where(first == 0.0, table * math.sqrt(0.5), table)


def cross_factors(order, to):
    half = order // 2
    block = cosine_table(order)[to * half:(to + 1) * half, (1 - to) * half:(2 - to) * half]
    even, odd = block[0::2], block[1::2]
    along = odd @ even.T / np.sum(even * even, axis=1)
    u, s, v = np.linalg.svd(odd - along @ even)
    kept = int(np.sum(s > 2.0 ** -24))
    v, u = v[:kept], u[:, :kept] * s[:kept]
    flip = np.sign(np.take_along_axis(v, np.argmax(np.abs(v), axis=1)[:, None], axis=1))
    count = even.shape[0]
    gather = np.concatenate([even, v * flip])
    spread = np.zeros((half, count + kept))
    spread[0::2, :count] = np.eye(count)
    spread[1::2, :count] = along
    spread[1::2, count:] = u * flip[:, 0]
    return gather, spread


def row_tables(order):
    half = order // 2
    table = cosine_table(order)
    near = np.stack([table[s * half:(s + 1) * half, s * half:(s + 1) * half] for s in range(2)])
    to_low, to_high = cross_factors(order, 0), cross_factors(order, 1)
    gather = np.stack([to_high[0], to_low[0]])
    spread = np.stack([to_low[1], to_high[1]])
    return tuple(jnp.asarray(t, jnp.float32).astype(jnp.bfloat16) for t in (near, gather, spread))


def build_column(right_ref, h_ref, scale):
    half = h_ref.shape[2]
    square = (LANES, LANES)
    inner = signs(iota(square, 0) & iota(square, 1), 7)

    def step(u, _):
        at = pl.ds(pl.multiple_of(u * LANES, LANES), LANES)
        for side in range(2):
            bits = right_ref[:, pl.ds(pl.multiple_of(side * half + u * LANES, LANES), LANES)]
            part = inner * down((2 * bits - 1).astype(jnp.float32) * scale)
            for v in range(half // LANES):
                common = u & v
                common = common ^ (common >> 4)
                common = common ^ (common >> 2)
                common = common ^ (common >> 1)
                sign = (1 - 2 * (common & 1)).astype(jnp.float32)
                q, c = v * LANES // SLAB, v * LANES % SLAB
                h_ref[side, q, at, c:c + LANES] = (part * sign).astype(jnp.bfloat16)
        return 0

    lax.fori_loop(0, half // LANES, step, 0)


def build_left(left_ref, left):
    def step(j, _):
        bits = left_ref[:, pl.ds(pl.multiple_of(j * HB, HB), HB)]
        left[j] = down((2 * bits - 1).astype(jnp.float32))
        return 0

    lax.fori_loop(0, left.shape[0], step, 0)


def expand(table, out_ref, mixed):
    high, wide = table.shape
    cuts = next(d for d in range(1, high + 1) if high % d == 0 and high // d * SUB <= LANES)
    chunk = high // cuts * SUB
    size = wide * SUB
    spread = (iota((size, wide), 0) // SUB == iota((size, wide), 1)).astype(jnp.float32).astype(jnp.bfloat16)
    if mixed:
        small = signs((iota((chunk, size), 0) & iota((chunk, size), 1)) & (SUB - 1), 4)
    else:
        small = (((iota((chunk, size), 0) ^ iota((chunk, size), 1)) & (SUB - 1)) == 0).astype(jnp.float32)

    def step(u, _):
        at = pl.multiple_of(u * chunk, chunk)
        here = ((at + iota((chunk, high), 0)) // SUB == iota((chunk, high), 1)).astype(jnp.float32)
        rows = jnp.dot(here.astype(jnp.bfloat16), table, preferred_element_type=jnp.float32)
        full = lax.dot_general(
            rows.astype(jnp.bfloat16), spread, (((1,), (1,)), ((), ())), preferred_element_type=jnp.float32
        )
        out_ref[pl.ds(at, chunk), :] = (full * small).astype(jnp.bfloat16)
        return 0

    lax.fori_loop(0, cuts, step, 0)


def build_order(p_ref):
    size = p_ref.shape[0]
    octets = SLAB // OCT

    def step(s, _):
        lane = iota((size, LANES), 1)
        wanted = lane // octets * SLAB + lane % octets * OCT + s
        hit = (wanted == iota((size, LANES), 0)).astype(jnp.float32)
        p_ref[:, pl.ds(pl.multiple_of(s * LANES, LANES), LANES)] = hit.astype(jnp.bfloat16)
        return 0

    lax.fori_loop(0, OCT, step, 0)


def fold_rows(parts):
    step = 1
    while step < len(parts):
        mixed = list(parts)
        for k in range(len(parts)):
            if not k & step:
                mixed[k] = parts[k] + parts[k + step]
                mixed[k + step] = parts[k] - parts[k + step]
        parts, step = mixed, 2 * step
    return parts


def loop(count, step):
    def run(i, _):
        step(i)
        return 0

    lax.fori_loop(0, count, run, 0)


def kernel(
    peers, experts, x_hbm, left_ref, right_ref, group_ref, near_ref, gather_ref, spread_ref,
    scaled_ref, error_ref, scale_ref, mean_ref, total_ref,
    x_ref, left, h_ref, near, gather, spread, p_ref, cols, out_s, in_s, planar_ref, planar_group, peaks,
    sum_ref, row_sums, expert_sums,
    send1, recv1, send2, recv2, send3, recv3, send_s, recv_s, send4, recv4, send5, recv5, load_sem,
):
    blocks, _, width = x_ref.shape
    half = width // 2
    slabs = width // SLAB
    pairs = slabs // 2
    mates = peers // 2
    rows = blocks * SUB
    me = lax.axis_index("row")
    mine = lax.axis_index("expert")
    side = me // mates
    slot = me - side * mates
    hub = mates - 1 + side
    far_hub = mates - side
    is_hub = me == hub
    hub_slot = hub - side * mates
    load = pltpu.make_async_copy(x_hbm, x_ref, load_sem)
    load.start()
    others = [lax.rem(me + d, peers) for d in range(1, peers)]
    elsewhere = [lax.rem(mine + d, experts) for d in range(1, experts)]
    mate_slots = [lax.rem(hub_slot + d, mates) for d in range(1, mates)]

    def remote(src, dst, send_sem, recv_sem, peer):
        return pltpu.make_async_remote_copy(
            src_ref=src, dst_ref=dst, send_sem=send_sem, recv_sem=recv_sem,
            device_id={"row": peer}, device_id_type=MESH,
        )

    def to_hub(s, k, who):
        piece = cols.at[s, k, who]
        return remote(piece, piece, send1.at[s, k], recv1.at[s, k, who], hub)

    def from_hub(s, k, who):
        return remote(
            cols.at[s, k, who], cols.at[s, k, hub_slot], send2.at[s, k, who], recv2.at[s, k],
            side * mates + who,
        )

    def across(s, k):
        return remote(out_s.at[s, k], in_s.at[s, k], send_s.at[s, k], recv_s.at[s, k], far_hub)

    def share_peak(t, s, peer):
        piece = peaks.at[t, s]
        return remote(piece, piece, send3.at[s, peer], recv3.at[t, s], peer)

    def copy4(peer, land):
        return remote(row_sums.at[me], row_sums.at[land], send4.at[peer], recv4.at[land], peer)

    def copy5(peer, land):
        return pltpu.make_async_remote_copy(
            src_ref=expert_sums.at[mine], dst_ref=expert_sums.at[land],
            send_sem=send5.at[peer], recv_sem=recv5.at[land],
            device_id={"expert": peer}, device_id_type=MESH,
        )

    barrier = pltpu.get_barrier_semaphore()
    for peer in others:
        pl.semaphore_signal(barrier, inc=1, device_id={"row": peer}, device_id_type=MESH)
    for peer in elsewhere:
        pl.semaphore_signal(barrier, inc=1, device_id={"expert": peer}, device_id_type=MESH)
    build_column(right_ref, h_ref, 1.0 / math.sqrt(width * HB))
    build_left(left_ref, left)
    load.wait()

    def column_side(q):
        def step(j):
            low = jnp.dot(x_ref[j, :, :half], h_ref[0, q], preferred_element_type=jnp.float32)
            high = jnp.dot(x_ref[j, :, half:], h_ref[1, q], preferred_element_type=jnp.float32)
            sign = jnp.concatenate([left[j]] * (SLAB // LANES), axis=1)
            for s, both in ((q, low + high), (q + pairs, low - high)):
                both = both * sign
                parts = fold_rows([both[k * SUB:(k + 1) * SUB] for k in range(FOLD)])
                for k in range(FOLD):
                    cols[s, k, slot, pl.ds(pl.multiple_of(j * SUB, SUB), SUB), :] = parts[k].astype(jnp.bfloat16)

        loop(blocks, step)

    def send_slab(s):
        loop(FOLD, lambda k: to_hub(s, k, slot).start())

    def forward(s, k):
        for who in mate_slots:
            to_hub(s, k, who).wait_recv()
        z = cols[s, k].reshape(mates * rows, SLAB)
        r = jnp.dot(gather[...], z, preferred_element_type=jnp.float32)
        out_s[s, k] = r.astype(jnp.bfloat16)
        across(s, k).start()

    def backward(s, k, peak):
        across(s, k).wait_recv()
        z = cols[s, k].reshape(mates * rows, SLAB)
        r = jnp.dot(near[...], z, preferred_element_type=jnp.float32)
        r = r + jnp.dot(spread[...], in_s[s, k], preferred_element_type=jnp.float32)
        cols[s, k] = r.astype(jnp.bfloat16).reshape(mates, rows, SLAB)
        for who in mate_slots:
            from_hub(s, k, who).start()
        return jnp.maximum(peak, jnp.max(jnp.abs(r).reshape(-1, 8, SLAB), axis=0))

    def group_scale(first, count):
        span = count * SLAB
        slab = [jnp.clip(first + i, 0, slabs - 1) for i in range(count)]
        top = jnp.concatenate([jnp.maximum(peaks[0, t], peaks[1, t])[:1] for t in slab], axis=1)
        group = jnp.concatenate(
            [group_ref[:, pl.ds(pl.multiple_of(t * SLAB, SLAB), SLAB)] for t in slab], axis=1
        )
        inside = group == iota((GROUPS, span), 0)
        return jnp.maximum(jnp.max(jnp.where(inside, top, 0.0), axis=1, keepdims=True), 1.0)

    total_rows = peers * blocks * HB

    def lattice(s):
        last = jnp.minimum(s + 1, slabs - 1)

        def peak_in(t):
            @pl.when(jnp.logical_or(jnp.logical_not(is_hub), side != t))
            def _():
                def wait(n):
                    share_peak(t, n, me).wait_recv()

                @pl.when(s == 0)
                def _():
                    wait(0)

                @pl.when(s + 1 < slabs)
                def _():
                    wait(last)

        for t in range(2):
            peak_in(t)
        factor = 2.0 / group_scale(s - 1, 3)
        at_slab = pl.ds(pl.multiple_of(s * SLAB, SLAB), SLAB)
        wide = group_ref[:, at_slab] == iota((GROUPS, SLAB), 0)
        natural = jnp.max(jnp.where(wide, factor, 0.0), axis=0, keepdims=True)
        wide = planar_group[s] == iota((GROUPS, OCT * LANES), 0).astype(jnp.float32)
        planar = jnp.max(jnp.where(wide, factor, 0.0), axis=0, keepdims=True)
        scales = [planar[:, c * LANES:(c + 1) * LANES] for c in range(OCT)]
        octets = SLAB // OCT
        lane = iota((SUB, LANES), 1)
        place = s % PACK
        here = lane // octets == place
        at_error = pl.ds(pl.multiple_of(s // PACK * LANES, LANES), LANES)

        def part(kk):
            @pl.when(jnp.logical_not(is_hub))
            def _():
                for g in range(PACK):
                    from_hub(s, kk * PACK + g, slot).wait_recv()

            both = jnp.concatenate([cols[s, kk * PACK + g, hub_slot] for g in range(PACK)], axis=1)
            planar_ref[...] = jnp.dot(both, p_ref[...], preferred_element_type=jnp.float32)

            def tile(j):
                at = pl.ds(pl.multiple_of(j * SUB, SUB), SUB)
                for g in range(PACK):
                    value = cols[s, kk * PACK + g, hub_slot, at, :].astype(jnp.float32) * natural
                    scaled_ref[j, kk * PACK + g, :, at_slab] = value.astype(jnp.bfloat16)
                square = near_sum = low = size = most = least = None
                for c in range(OCT):
                    value = planar_ref[at, c * LANES:(c + 1) * LANES] * scales[c]
                    nearest = jnp.round(value)
                    offset = jnp.abs(value - nearest)
                    below = jnp.floor(value)
                    if c == 0:
                        square, near_sum, low, size = offset * offset, nearest, below, offset
                        most = least = offset
                    else:
                        square, near_sum, low = square + offset * offset, near_sum + nearest, low + below
                        size = size + offset
                        most, least = jnp.maximum(most, offset), jnp.minimum(least, offset)
                odd = near_sum - 2.0 * jnp.floor(near_sum * 0.5) > 0.5
                whole = jnp.where(odd, square + (1.0 - 2.0 * most), square)
                shifted = square + (OCT * 0.25 - size)
                odd = low - 2.0 * jnp.floor(low * 0.5) > 0.5
                error = jnp.minimum(whole, jnp.where(odd, shifted + 2.0 * least, shifted))
                row = me * (blocks * HB) + j * HB + (kk * PACK + lane // octets) * SUB + iota((SUB, LANES), 0)
                weight = (1.0 + 4.0 * (row.astype(jnp.float32) + 0.5) / total_rows) / 3.0
                sum_ref[...] += error * weight
                for g in range(PACK):
                    turned = pltpu.roll(error, lax.rem(place + PACK - g, PACK) * octets, 1)
                    old = error_ref[j, kk * PACK + g, :, at_error]
                    error_ref[j, kk * PACK + g, :, at_error] = jnp.where(here, turned, old)

            loop(blocks, tile)

        loop(FOLD // PACK, part)

    column_side(0)
    pl.semaphore_wait(barrier, peers + experts - 2)

    @pl.when(jnp.logical_not(is_hub))
    def _():
        send_slab(0)

        def step(q):
            column_side(q + 1)
            send_slab(q + 1)

        loop(pairs - 1, step)
        loop(slabs - pairs, lambda q: send_slab(q + pairs))

    @pl.when(is_hub)
    def _():
        expand(gather_ref[side], gather, True)
        expand(near_ref[side], near, True)
        expand(spread_ref[side], spread, False)
        loop(FOLD, lambda k: forward(0, k))

    build_order(p_ref)
    sum_ref[...] = jnp.zeros_like(sum_ref)

    def group_order(s):
        row = group_ref[:, pl.ds(pl.multiple_of(s * SLAB, SLAB), SLAB)].astype(jnp.float32)
        row = jnp.concatenate([jnp.broadcast_to(row, (SUB, SLAB)).astype(jnp.bfloat16)] * PACK, axis=1)
        planar_group[s] = jnp.dot(row, p_ref[...], preferred_element_type=jnp.float32)[:1]

    loop(slabs, group_order)

    def stage(t):
        @pl.when(jnp.logical_and(is_hub, t + 1 < pairs))
        def _():
            column_side(t + 1)

        @pl.when(t >= 2)
        def _():
            lattice(t - 2)

        @pl.when(jnp.logical_and(is_hub, t < slabs))
        def _():
            def step(k, peak):
                @pl.when(t + 1 < slabs)
                def _():
                    forward(t + 1, k)

                return backward(t, k, peak)

            peak = lax.fori_loop(0, FOLD, step, jnp.zeros((8, SLAB), jnp.float32))
            peaks[side, t] = jnp.broadcast_to(jnp.max(peak, axis=0, keepdims=True), (8, SLAB))
            for peer in others:
                share_peak(side, t, peer).start()

    loop(slabs + 2, stage)

    peak = group_scale(0, slabs) * 0.5
    scale_ref[...] = jnp.broadcast_to(peak, (GROUPS, LANES)).T[:1, :GROUPS]

    part = jnp.sum(jnp.sum(sum_ref[...], axis=0, keepdims=True), axis=1, keepdims=True)
    row_sums[me] = jnp.broadcast_to(part / (total_rows * width // OCT), (8, LANES))
    for peer in others:
        copy4(peer, me).start()
    for peer in others:
        copy4(peer, peer).wait_recv()
    mean = row_sums[0]
    for q in range(1, peers):
        mean = mean + row_sums[q]
    expert_sums[mine] = mean
    for peer in elsewhere:
        copy5(peer, mine).start()
    for peer in elsewhere:
        copy5(peer, peer).wait_recv()
    total = expert_sums[0]
    for e in range(1, experts):
        total = total + expert_sums[e]
    mean_ref[0] = jnp.max(mean)
    total_ref[0] = jnp.max(total / experts)

    @pl.when(jnp.logical_not(is_hub))
    def _():
        loop(slabs, lambda s: loop(FOLD, lambda k: to_hub(s, k, slot).wait_send()))

    @pl.when(is_hub)
    def _():
        def drain(s):
            for peer in others:
                share_peak(side, s, peer).wait_send()

            def step(k):
                across(s, k).wait_send()
                for who in mate_slots:
                    from_hub(s, k, who).wait_send()

            loop(FOLD, step)

        loop(slabs, drain)

    for peer in others:
        copy4(peer, me).wait_send()
    for peer in elsewhere:
        copy5(peer, mine).wait_send()


def put_kernel(scaled_ref, error_ref, scaled_out, error_out, sems):
    copies = (
        pltpu.make_async_copy(scaled_ref, scaled_out, sems.at[0]),
        pltpu.make_async_copy(error_ref, error_out, sems.at[1]),
    )
    for copy in copies:
        copy.start()
    for copy in copies:
        copy.wait()


def put(scaled, errors):
    return pl.pallas_call(
        put_kernel,
        out_shape=(
            jax.ShapeDtypeStruct(scaled.shape, scaled.dtype),
            jax.ShapeDtypeStruct(errors.shape, errors.dtype),
        ),
        in_specs=[pl.BlockSpec(memory_space=pltpu.VMEM)] * 2,
        out_specs=[pl.BlockSpec(memory_space=pl.ANY)] * 2,
        scratch_shapes=[pltpu.SemaphoreType.DMA((2,))],
        compiler_params=pltpu.CompilerParams(vmem_limit_bytes=16 * 2**20),
    )(scaled, errors)


def body(weights, left_bits, right_bits, groups):
    _, local_rows, width = weights.shape
    peers = lax.axis_size("row")
    experts = lax.axis_size("expert")
    blocks = local_rows // HB
    half = width // 2
    mates = peers // 2
    rows = blocks * SUB
    slabs = width // SLAB
    near, gather, spread = row_tables(BLOCKS)
    inner, reach = mates * rows, gather.shape[1] * SUB
    vmem = pl.BlockSpec(memory_space=pltpu.VMEM)
    hbm = pl.BlockSpec(memory_space=pl.ANY)
    dma = pltpu.SemaphoreType.DMA
    smem = pl.BlockSpec(memory_space=pltpu.SMEM)
    scaled, errors, group_scale, mean, total = pl.pallas_call(
        functools.partial(kernel, peers, experts),
        out_shape=(
            pltpu.VMEM((blocks, FOLD, SUB, width), jnp.bfloat16),
            pltpu.VMEM((blocks, FOLD, SUB, width // OCT), jnp.float32),
            jax.ShapeDtypeStruct((1, GROUPS), jnp.float32),
            jax.ShapeDtypeStruct((1,), jnp.float32),
            jax.ShapeDtypeStruct((1,), jnp.float32),
        ),
        in_specs=[hbm] + [vmem] * 6,
        out_specs=(vmem, vmem, vmem, smem, smem),
        scratch_shapes=[
            pltpu.VMEM((blocks, HB, width), jnp.bfloat16),
            pltpu.VMEM((blocks, HB, LANES), jnp.float32),
            pltpu.VMEM((2, slabs // 2, half, SLAB), jnp.bfloat16),
            pltpu.VMEM((inner, inner), jnp.bfloat16),
            pltpu.VMEM((reach, inner), jnp.bfloat16),
            pltpu.VMEM((inner, reach), jnp.bfloat16),
            pltpu.VMEM((PACK * SLAB, OCT * LANES), jnp.bfloat16),
            pltpu.VMEM((slabs, FOLD, mates, rows, SLAB), jnp.bfloat16),
            pltpu.VMEM((slabs, FOLD, reach, SLAB), jnp.bfloat16),
            pltpu.VMEM((slabs, FOLD, reach, SLAB), jnp.bfloat16),
            pltpu.VMEM((rows, OCT * LANES), jnp.float32),
            pltpu.VMEM((slabs, 1, OCT * LANES), jnp.float32),
            pltpu.VMEM((2, slabs, 8, SLAB), jnp.float32),
            pltpu.VMEM((SUB, LANES), jnp.float32),
            pltpu.VMEM((peers, 8, LANES), jnp.float32),
            pltpu.VMEM((experts, 8, LANES), jnp.float32),
            dma((slabs, FOLD)),
            dma((slabs, FOLD, mates)),
            dma((slabs, FOLD, mates)),
            dma((slabs, FOLD)),
            dma((slabs, peers)),
            dma((2, slabs)),
            dma((slabs, FOLD)),
            dma((slabs, FOLD)),
            dma((peers,)),
            dma((peers,)),
            dma((experts,)),
            dma((experts,)),
            dma,
        ],
        compiler_params=pltpu.CompilerParams(
            collective_id=0, has_side_effects=True, vmem_limit_bytes=54 * 2**20
        ),
    )(weights.reshape(blocks, HB, width), left_bits, right_bits, groups, near, gather, spread)
    scaled, errors = put(scaled, errors)
    return (
        scaled.reshape(1, local_rows, width),
        errors.reshape(1, local_rows, width // OCT),
        group_scale,
        mean,
        total.reshape(()),
    )


def solution(mesh):
    placed = (P("expert", "row", None), P("expert", "row"), P("expert", None), P("expert", None))
    return jax.shard_map(
        body,
        mesh=mesh,
        in_specs=placed,
        out_specs=(
            P("expert", "row", None),
            P("expert", "row", None),
            P("expert", None),
            P("expert"),
            P(),
        ),
        check_vma=False,
    )
```

```python
import functools
import math

import jax
import jax.numpy as jnp
import numpy as np
from jax import lax
from jax.experimental import pallas as pl
from jax.experimental.pallas import tpu as pltpu
from jax.sharding import PartitionSpec as P

HB = 128
SUB = 16
FOLD = HB // SUB
OCT = 8
LANES = 128
GROUPS = 16
BLOCKS = 56
SLAB = 256
PACK = LANES * OCT // SLAB
LEAD = 3
MESH = pl.DeviceIdType.MESH


def signs(common, bits):
    for shift in (4, 2, 1):
        if shift < bits:
            common = common ^ (common >> shift)
    return (1 - 2 * (common & 1)).astype(jnp.float32)


def iota(shape, dim):
    return lax.broadcasted_iota(jnp.int32, shape, dim)


def down(row):
    return jnp.broadcast_to(row, (LANES, LANES)).T


def cosine_table(order):
    first = np.arange(order, dtype=np.float64)[:, None]
    second = np.arange(order, dtype=np.float64)[None, :]
    table = math.sqrt(2.0 / order) * np.cos(math.pi * (2.0 * second + 1.0) * first / (2.0 * order))
    return np.where(first == 0.0, table * math.sqrt(0.5), table)


def cross_factors(order, to):
    half = order // 2
    block = cosine_table(order)[to * half:(to + 1) * half, (1 - to) * half:(2 - to) * half]
    even, odd = block[0::2], block[1::2]
    along = odd @ even.T / np.sum(even * even, axis=1)
    u, s, v = np.linalg.svd(odd - along @ even)
    kept = int(np.sum(s > 2.0 ** -24))
    v, u = v[:kept], u[:, :kept] * s[:kept]
    flip = np.sign(np.take_along_axis(v, np.argmax(np.abs(v), axis=1)[:, None], axis=1))
    count = even.shape[0]
    gather = np.concatenate([even, v * flip])
    spread = np.zeros((half, count + kept))
    spread[0::2, :count] = np.eye(count)
    spread[1::2, :count] = along
    spread[1::2, count:] = u * flip[:, 0]
    return gather, spread


def row_tables(order):
    half = order // 2
    table = cosine_table(order)
    near = np.stack([table[s * half:(s + 1) * half, s * half:(s + 1) * half] for s in range(2)])
    to_low, to_high = cross_factors(order, 0), cross_factors(order, 1)
    gather = np.stack([to_high[0], to_low[0]])
    spread = np.stack([to_low[1], to_high[1]])
    index = np.arange(SUB)
    inner = np.array([[1 - 2 * (bin(a & b).count("1") & 1) for b in index] for a in index], np.float32)
    return tuple(
        np.stack([np.kron(t, m) for t in ts]).astype(np.float32).astype(np.dtype(jnp.bfloat16))
        for ts, m in ((near, inner), (gather, inner), (spread, np.eye(SUB, dtype=np.float32)))
    )


def build_column(right_ref, h_ref, scale):
    half = h_ref.shape[2]
    square = (LANES, LANES)
    inner = signs(iota(square, 0) & iota(square, 1), 7)

    def step(u, _):
        at = pl.ds(pl.multiple_of(u * LANES, LANES), LANES)
        for side in range(2):
            bits = right_ref[:, pl.ds(pl.multiple_of(side * half + u * LANES, LANES), LANES)]
            part = inner * down((2 * bits - 1).astype(jnp.float32) * scale)
            for v in range(half // LANES):
                common = u & v
                common = common ^ (common >> 4)
                common = common ^ (common >> 2)
                common = common ^ (common >> 1)
                sign = (1 - 2 * (common & 1)).astype(jnp.float32)
                q, c = v * LANES // SLAB, v * LANES % SLAB
                h_ref[side, q, at, c:c + LANES] = (part * sign).astype(jnp.bfloat16)
        return 0

    lax.fori_loop(0, half // LANES, step, 0)


def build_left(left_ref, left):
    def step(j, _):
        bits = left_ref[:, pl.ds(pl.multiple_of(j * HB, HB), HB)]
        left[j] = down((2 * bits - 1).astype(jnp.float32))
        return 0

    lax.fori_loop(0, left.shape[0], step, 0)


def build_order(p_ref):
    size = p_ref.shape[0]
    octets = SLAB // OCT

    def step(s, _):
        lane = iota((size, LANES), 1)
        wanted = lane // octets * SLAB + lane % octets * OCT + s
        hit = (wanted == iota((size, LANES), 0)).astype(jnp.float32)
        p_ref[:, pl.ds(pl.multiple_of(s * LANES, LANES), LANES)] = hit.astype(jnp.bfloat16)
        return 0

    lax.fori_loop(0, OCT, step, 0)


def fold_rows(parts):
    step = 1
    while step < len(parts):
        mixed = list(parts)
        for k in range(len(parts)):
            if not k & step:
                mixed[k] = parts[k] + parts[k + step]
                mixed[k + step] = parts[k] - parts[k + step]
        parts, step = mixed, 2 * step
    return parts


def loop(count, step):
    def run(i, _):
        step(i)
        return 0

    lax.fori_loop(0, count, run, 0)


def kernel(
    peers, experts, x_hbm, left_hbm, right_hbm, group_hbm, near_hbm, gather_hbm, spread_hbm,
    scaled_ref, error_ref, scale_ref, mean_ref, total_ref,
    x_ref, left_ref, right_ref, group_ref, near, gather, spread,
    left, h_ref, p_ref, cols, out_s, in_s, planar_ref, planar_group, peaks, peak_ref, natural_ref, factor_ref,
    sum_ref, sums,
    send1, recv1, send2, recv2, send3, recv3, send_s, recv_s, send4, recv4, load_sem,
):
    blocks, _, width = x_ref.shape
    half = width // 2
    slabs = width // SLAB
    pairs = slabs // 2
    mates = peers // 2
    rows = blocks * SUB
    me = lax.axis_index("row")
    mine = lax.axis_index("expert")
    side = me // mates
    slot = me - side * mates
    hub = mates - 1 + side
    far_hub = mates - side
    is_hub = me == hub
    hub_slot = hub - side * mates
    loads = [
        pltpu.make_async_copy(src, dst, load_sem.at[n])
        for n, (src, dst) in enumerate((
            (right_hbm, right_ref), (left_hbm, left_ref), (x_hbm, x_ref), (group_hbm, group_ref),
            (gather_hbm.at[side], gather), (near_hbm.at[side], near), (spread_hbm.at[side], spread),
        ))
    ]
    for load in loads:
        load.start()
    others = [lax.rem(me + d, peers) for d in range(1, peers)]
    devices = peers * experts
    here = mine * peers + me
    mate_slots = [lax.rem(hub_slot + d, mates) for d in range(1, mates)]

    def remote(src, dst, send_sem, recv_sem, peer):
        return pltpu.make_async_remote_copy(
            src_ref=src, dst_ref=dst, send_sem=send_sem, recv_sem=recv_sem,
            device_id={"row": peer}, device_id_type=MESH,
        )

    def to_hub(s, k, who):
        piece = cols.at[s, k, who]
        return remote(piece, piece, send1.at[s, k], recv1.at[s, k, who], hub)

    def from_hub(s, k, who):
        return remote(
            cols.at[s, k, who], cols.at[s, k, hub_slot], send2.at[s, k, who], recv2.at[s, k],
            side * mates + who,
        )

    def across(s, k):
        return remote(out_s.at[s, k], in_s.at[s, k], send_s.at[s, k], recv_s.at[s, k], far_hub)

    def share_peak(t, s, peer):
        piece = peaks.at[t, s]
        return remote(piece, piece, send3.at[s, peer], recv3.at[t, s], peer)

    def share_sum(n, land):
        there = lax.rem(here + n, devices)
        return pltpu.make_async_remote_copy(
            src_ref=sums.at[here], dst_ref=sums.at[land], send_sem=send4.at[there], recv_sem=recv4.at[land],
            device_id={"expert": there // peers, "row": lax.rem(there, peers)}, device_id_type=MESH,
        )

    barrier = pltpu.get_barrier_semaphore()

    def greet(n):
        there = lax.rem(here + n + 1, devices)
        pl.semaphore_signal(
            barrier, inc=1, device_id={"expert": there // peers, "row": lax.rem(there, peers)}, device_id_type=MESH
        )

    loop(devices - 1, greet)
    loads[0].wait()
    build_column(right_ref, h_ref, 1.0 / math.sqrt(width * HB))
    loads[1].wait()
    build_left(left_ref, left)
    loads[2].wait()

    def column_side(q):
        def step(j):
            low = jnp.dot(x_ref[j, :, :half], h_ref[0, q], preferred_element_type=jnp.float32)
            high = jnp.dot(x_ref[j, :, half:], h_ref[1, q], preferred_element_type=jnp.float32)
            sign = jnp.concatenate([left[j]] * (SLAB // LANES), axis=1)
            for s, both in ((q, low + high), (q + pairs, low - high)):
                both = both * sign
                parts = fold_rows([both[k * SUB:(k + 1) * SUB] for k in range(FOLD)])
                for k in range(FOLD):
                    cols[s, k, slot, pl.ds(pl.multiple_of(j * SUB, SUB), SUB), :] = parts[k].astype(jnp.bfloat16)

        loop(blocks, step)

    def send_slab(s):
        loop(FOLD, lambda k: to_hub(s, k, slot).start())

    def forward(s, k):
        for who in mate_slots:
            to_hub(s, k, who).wait_recv()
        z = cols[s, k].reshape(mates * rows, SLAB)
        r = jnp.dot(gather[...], z, preferred_element_type=jnp.float32)
        out_s[s, k] = r.astype(jnp.bfloat16)
        across(s, k).start()

    def backward(s, k):
        across(s, k).wait_recv()
        z = cols[s, k].reshape(mates * rows, SLAB)
        r = jnp.dot(near[...], z, preferred_element_type=jnp.float32)
        r = r + jnp.dot(spread[...], in_s[s, k], preferred_element_type=jnp.float32)
        cols[s, k] = r.astype(jnp.bfloat16).reshape(mates, rows, SLAB)
        for who in mate_slots:
            from_hub(s, k, who).start()
        peak_ref[...] = jnp.maximum(peak_ref[...], jnp.max(jnp.abs(r).reshape(-1, 8, SLAB), axis=0))

    def group_scale(first, count):
        span = count * SLAB
        slab = [jnp.clip(first + i, 0, slabs - 1) for i in range(count)]
        top = jnp.concatenate([jnp.maximum(peaks[0, t], peaks[1, t])[:1] for t in slab], axis=1)
        group = jnp.concatenate(
            [group_ref[:, pl.ds(pl.multiple_of(t * SLAB, SLAB), SLAB)] for t in slab], axis=1
        )
        inside = group == iota((GROUPS, span), 0)
        return jnp.maximum(jnp.max(jnp.where(inside, top, 0.0), axis=1, keepdims=True), 1.0)

    total_rows = peers * blocks * HB
    unroll = next(u for u in (2, 1) if blocks % u == 0)

    def scale_slab(s):
        last = jnp.minimum(s + 1, slabs - 1)

        def peak_in(t):
            @pl.when(jnp.logical_or(jnp.logical_not(is_hub), side != t))
            def _():
                @pl.when(s == 0)
                def _():
                    share_peak(t, 0, me).wait_recv()

                @pl.when(s + 1 < slabs)
                def _():
                    share_peak(t, last, me).wait_recv()

        for t in range(2):
            peak_in(t)
        factor = 2.0 / group_scale(s - 1, 3)
        wide = group_ref[:, pl.ds(pl.multiple_of(s * SLAB, SLAB), SLAB)] == iota((GROUPS, SLAB), 0)
        natural_ref[...] = jnp.max(jnp.where(wide, factor, 0.0), axis=0, keepdims=True)
        wide = planar_group[pl.ds(s, 1), :] == iota((GROUPS, OCT * LANES), 0).astype(jnp.float32)
        factor_ref[...] = jnp.max(jnp.where(wide, factor, 0.0), axis=0, keepdims=True)

    def lattice(s, kk):
        at_slab = pl.ds(pl.multiple_of(s * SLAB, SLAB), SLAB)
        octets = SLAB // OCT
        lane = iota((SUB, LANES), 1)
        place = s % PACK
        inside = lane // octets == place
        at_error = pl.ds(pl.multiple_of(s // PACK * LANES, LANES), LANES)
        first = (me * (blocks * HB) + (kk * PACK + lane // octets) * SUB + iota((SUB, LANES), 0)).astype(jnp.float32)

        @pl.when(jnp.logical_not(is_hub))
        def _():
            for g in range(PACK):
                from_hub(s, kk * PACK + g, slot).wait_recv()

        both = jnp.concatenate([cols[s, kk * PACK + g, hub_slot] for g in range(PACK)], axis=1)
        planar_ref[...] = jnp.dot(both, p_ref[...], preferred_element_type=jnp.float32)

        def tile(j):
            at = pl.ds(pl.multiple_of(j * SUB, SUB), SUB)
            natural = natural_ref[...]
            for g in range(PACK):
                value = cols[s, kk * PACK + g, hub_slot, at, :].astype(jnp.float32) * natural
                scaled_ref[j, kk * PACK + g, :, at_slab] = value.astype(jnp.bfloat16)
            square = near_sum = low = size = most = least = None
            for c in range(OCT):
                value = planar_ref[at, c * LANES:(c + 1) * LANES] * factor_ref[:, c * LANES:(c + 1) * LANES]
                nearest = jnp.round(value)
                offset = jnp.abs(value - nearest)
                below = jnp.floor(value)
                if c == 0:
                    square, near_sum, low, size = offset * offset, nearest, below, offset
                    most = least = offset
                else:
                    square, near_sum, low = square + offset * offset, near_sum + nearest, low + below
                    size = size + offset
                    most, least = jnp.maximum(most, offset), jnp.minimum(least, offset)
            odd = near_sum - 2.0 * jnp.floor(near_sum * 0.5) > 0.5
            whole = jnp.where(odd, square + (1.0 - 2.0 * most), square)
            shifted = square + (OCT * 0.25 - size)
            odd = low - 2.0 * jnp.floor(low * 0.5) > 0.5
            error = jnp.minimum(whole, jnp.where(odd, shifted + 2.0 * least, shifted))
            for g in range(PACK):
                turned = pltpu.roll(error, lax.rem(place + PACK - g, PACK) * octets, 1)
                old = error_ref[j, kk * PACK + g, :, at_error]
                error_ref[j, kk * PACK + g, :, at_error] = jnp.where(inside, turned, old)
            row = first + (j * HB).astype(jnp.float32)
            return error * ((1.0 + 4.0 * (row + 0.5) / total_rows) / 3.0)

        def some(i):
            parts = [tile(i * unroll + u) for u in range(unroll)]
            sum_ref[...] += sum(parts[1:], parts[0])

        loop(blocks // unroll, some)

    column_side(0)
    pl.semaphore_wait(barrier, devices - 1)

    @pl.when(jnp.logical_not(is_hub))
    def _():
        send_slab(0)

        def step(q):
            column_side(q + 1)
            send_slab(q + 1)

        loop(pairs - 1, step)
        loop(slabs - pairs, lambda q: send_slab(q + pairs))

    for load in loads[3:]:
        load.wait()

    @pl.when(is_hub)
    def _():
        loop(LEAD, lambda k: forward(0, k))

    build_order(p_ref)
    sum_ref[...] = jnp.zeros_like(sum_ref)
    row = jnp.concatenate([group_ref[:, s * SLAB:(s + 1) * SLAB] for s in range(slabs)], axis=0)
    row = jnp.concatenate([row.astype(jnp.float32).astype(jnp.bfloat16)] * PACK, axis=1)
    planar_group[...] = jnp.dot(row, p_ref[...], preferred_element_type=jnp.float32)

    def stage(t):
        mixes = jnp.logical_and(is_hub, t < slabs)

        @pl.when(mixes)
        def _():
            peak_ref[...] = jnp.zeros_like(peak_ref)

        @pl.when(jnp.logical_and(is_hub, t + 1 < pairs))
        def _():
            column_side(t + 1)

        def part(kk):
            @pl.when(mixes)
            def _():
                def step(i):
                    k = kk * PACK + i
                    ahead = t * FOLD + k + LEAD

                    @pl.when(ahead < slabs * FOLD)
                    def _():
                        forward(ahead // FOLD, ahead % FOLD)

                    backward(t, k)

                loop(PACK, step)

            @pl.when(t >= 2)
            def _():
                @pl.when(kk == 0)
                def _():
                    scale_slab(t - 2)

                lattice(t - 2, kk)

        loop(FOLD // PACK, part)

        @pl.when(mixes)
        def _():
            peaks[side, t] = jnp.broadcast_to(jnp.max(peak_ref[...], axis=0, keepdims=True), (8, SLAB))
            for peer in others:
                share_peak(side, t, peer).start()

    loop(slabs + 2, stage)

    peak = group_scale(0, slabs) * 0.5
    scale_ref[...] = jnp.broadcast_to(peak, (GROUPS, LANES)).T[:1, :GROUPS]

    part = jnp.sum(jnp.sum(sum_ref[...], axis=0, keepdims=True), axis=1, keepdims=True)
    sums[here] = jnp.broadcast_to(part / (total_rows * width // OCT), (1, LANES))
    loop(devices - 1, lambda n: share_sum(n + 1, here).start())

    def wait_sum(n):
        land = lax.rem(here + n + 1, devices)
        share_sum(n + 1, land).wait_recv()

    loop(devices - 1, wait_sum)
    total = jnp.sum(sums[...], axis=0)
    mean = jnp.sum(sums[pl.ds(mine * peers, peers)], axis=0)
    mean_ref[0] = jnp.max(mean)
    total_ref[0] = jnp.max(total / experts)

    @pl.when(jnp.logical_not(is_hub))
    def _():
        loop(slabs, lambda s: loop(FOLD, lambda k: to_hub(s, k, slot).wait_send()))

    @pl.when(is_hub)
    def _():
        def drain(s):
            for peer in others:
                share_peak(side, s, peer).wait_send()

            def step(k):
                across(s, k).wait_send()
                for who in mate_slots:
                    from_hub(s, k, who).wait_send()

            loop(FOLD, step)

        loop(slabs, drain)

    loop(devices - 1, lambda n: share_sum(n + 1, here).wait_send())


def put_kernel(scaled_ref, error_ref, scaled_out, error_out, sems):
    copies = (
        pltpu.make_async_copy(scaled_ref, scaled_out, sems.at[0]),
        pltpu.make_async_copy(error_ref, error_out, sems.at[1]),
    )
    for copy in copies:
        copy.start()
    for copy in copies:
        copy.wait()


def put(scaled, errors):
    return pl.pallas_call(
        put_kernel,
        out_shape=(
            jax.ShapeDtypeStruct(scaled.shape, scaled.dtype),
            jax.ShapeDtypeStruct(errors.shape, errors.dtype),
        ),
        in_specs=[pl.BlockSpec(memory_space=pltpu.VMEM)] * 2,
        out_specs=[pl.BlockSpec(memory_space=pl.ANY)] * 2,
        scratch_shapes=[pltpu.SemaphoreType.DMA((2,))],
        compiler_params=pltpu.CompilerParams(vmem_limit_bytes=16 * 2**20),
    )(scaled, errors)


def body(weights, left_bits, right_bits, groups):
    _, local_rows, width = weights.shape
    peers = lax.axis_size("row")
    experts = lax.axis_size("expert")
    blocks = local_rows // HB
    half = width // 2
    mates = peers // 2
    rows = blocks * SUB
    slabs = width // SLAB
    near, gather, spread = row_tables(BLOCKS)
    inner, reach = mates * rows, gather.shape[1]
    vmem = pl.BlockSpec(memory_space=pltpu.VMEM)
    hbm = pl.BlockSpec(memory_space=pl.ANY)
    dma = pltpu.SemaphoreType.DMA
    smem = pl.BlockSpec(memory_space=pltpu.SMEM)
    scaled, errors, group_scale, mean, total = pl.pallas_call(
        functools.partial(kernel, peers, experts),
        out_shape=(
            pltpu.VMEM((blocks, FOLD, SUB, width), jnp.bfloat16),
            pltpu.VMEM((blocks, FOLD, SUB, width // OCT), jnp.float32),
            jax.ShapeDtypeStruct((1, GROUPS), jnp.float32),
            jax.ShapeDtypeStruct((1,), jnp.float32),
            jax.ShapeDtypeStruct((1,), jnp.float32),
        ),
        in_specs=[hbm] * 7,
        out_specs=(vmem, vmem, vmem, smem, smem),
        scratch_shapes=[
            pltpu.VMEM((blocks, HB, width), jnp.bfloat16),
            pltpu.VMEM((1, local_rows), jnp.int32),
            pltpu.VMEM((1, width), jnp.int32),
            pltpu.VMEM((1, width), jnp.int32),
            pltpu.VMEM((inner, inner), jnp.bfloat16),
            pltpu.VMEM((reach, inner), jnp.bfloat16),
            pltpu.VMEM((inner, reach), jnp.bfloat16),
            pltpu.VMEM((blocks, HB, LANES), jnp.float32),
            pltpu.VMEM((2, slabs // 2, half, SLAB), jnp.bfloat16),
            pltpu.VMEM((PACK * SLAB, OCT * LANES), jnp.bfloat16),
            pltpu.VMEM((slabs, FOLD, mates, rows, SLAB), jnp.bfloat16),
            pltpu.VMEM((slabs, FOLD, reach, SLAB), jnp.bfloat16),
            pltpu.VMEM((slabs, FOLD, reach, SLAB), jnp.bfloat16),
            pltpu.VMEM((rows, OCT * LANES), jnp.float32),
            pltpu.VMEM((slabs, OCT * LANES), jnp.float32),
            pltpu.VMEM((2, slabs, 8, SLAB), jnp.float32),
            pltpu.VMEM((8, SLAB), jnp.float32),
            pltpu.VMEM((1, SLAB), jnp.float32),
            pltpu.VMEM((1, OCT * LANES), jnp.float32),
            pltpu.VMEM((SUB, LANES), jnp.float32),
            pltpu.VMEM((peers * experts, 1, LANES), jnp.float32),
            dma((slabs, FOLD)),
            dma((slabs, FOLD, mates)),
            dma((slabs, FOLD, mates)),
            dma((slabs, FOLD)),
            dma((slabs, peers)),
            dma((2, slabs)),
            dma((slabs, FOLD)),
            dma((slabs, FOLD)),
            dma((peers * experts,)),
            dma((peers * experts,)),
            dma((7,)),
        ],
        compiler_params=pltpu.CompilerParams(
            collective_id=0, has_side_effects=True, vmem_limit_bytes=54 * 2**20
        ),
    )(weights.reshape(blocks, HB, width), left_bits, right_bits, groups, near, gather, spread)
    scaled, errors = put(scaled, errors)
    return (
        scaled.reshape(1, local_rows, width),
        errors.reshape(1, local_rows, width // OCT),
        group_scale,
        mean,
        total.reshape(()),
    )


def solution(mesh):
    placed = (P("expert", "row", None), P("expert", "row"), P("expert", None), P("expert", None))
    return jax.shard_map(
        body,
        mesh=mesh,
        in_specs=placed,
        out_specs=(
            P("expert", "row", None),
            P("expert", "row", None),
            P("expert", None),
            P("expert"),
            P(),
        ),
        check_vma=False,
    )
```

```python
import functools
import math

import jax
import jax.numpy as jnp
import numpy as np
from jax import lax
from jax.experimental import pallas as pl
from jax.experimental.pallas import tpu as pltpu
from jax.sharding import PartitionSpec as P

HB = 128
SUB = 16
FOLD = HB // SUB
OCT = 8
LANES = 128
GROUPS = 16
BLOCKS = 56
SLAB = 256
PACK = LANES * OCT // SLAB
LEAD = 3
MESH = pl.DeviceIdType.MESH


def signs(common, bits):
    for shift in (4, 2, 1):
        if shift < bits:
            common = common ^ (common >> shift)
    return (1 - 2 * (common & 1)).astype(jnp.float32)


def iota(shape, dim):
    return lax.broadcasted_iota(jnp.int32, shape, dim)


def down(row):
    return jnp.broadcast_to(row, (LANES, LANES)).T


def cosine_table(order):
    first = np.arange(order, dtype=np.float64)[:, None]
    second = np.arange(order, dtype=np.float64)[None, :]
    table = math.sqrt(2.0 / order) * np.cos(math.pi * (2.0 * second + 1.0) * first / (2.0 * order))
    return np.where(first == 0.0, table * math.sqrt(0.5), table)


def cross_factors(order, to):
    half = order // 2
    block = cosine_table(order)[to * half:(to + 1) * half, (1 - to) * half:(2 - to) * half]
    even, odd = block[0::2], block[1::2]
    along = odd @ even.T / np.sum(even * even, axis=1)
    u, s, v = np.linalg.svd(odd - along @ even)
    kept = int(np.sum(s > 2.0 ** -24))
    v, u = v[:kept], u[:, :kept] * s[:kept]
    flip = np.sign(np.take_along_axis(v, np.argmax(np.abs(v), axis=1)[:, None], axis=1))
    count = even.shape[0]
    gather = np.concatenate([even, v * flip])
    spread = np.zeros((half, count + kept))
    spread[0::2, :count] = np.eye(count)
    spread[1::2, :count] = along
    spread[1::2, count:] = u * flip[:, 0]
    return gather, spread


def row_tables(order):
    half = order // 2
    table = cosine_table(order)
    near = np.stack([table[s * half:(s + 1) * half, s * half:(s + 1) * half] for s in range(2)])
    to_low, to_high = cross_factors(order, 0), cross_factors(order, 1)
    gather = np.stack([to_high[0], to_low[0]])
    spread = np.stack([to_low[1], to_high[1]])
    index = np.arange(SUB)
    inner = np.array([[1 - 2 * (bin(a & b).count("1") & 1) for b in index] for a in index], np.float32)
    return tuple(
        np.stack([np.kron(t, m) for t in ts]).astype(np.float32).astype(np.dtype(jnp.bfloat16))
        for ts, m in ((near, inner), (gather, inner), (spread, np.eye(SUB, dtype=np.float32)))
    )


def build_column(right_ref, h_ref, scale):
    half = h_ref.shape[2]
    square = (LANES, LANES)
    inner = signs(iota(square, 0) & iota(square, 1), 7)

    def step(u, _):
        at = pl.ds(pl.multiple_of(u * LANES, LANES), LANES)
        for side in range(2):
            bits = right_ref[:, pl.ds(pl.multiple_of(side * half + u * LANES, LANES), LANES)]
            part = inner * down((2 * bits - 1).astype(jnp.float32) * scale)
            for v in range(half // LANES):
                common = u & v
                common = common ^ (common >> 4)
                common = common ^ (common >> 2)
                common = common ^ (common >> 1)
                sign = (1 - 2 * (common & 1)).astype(jnp.float32)
                q, c = v * LANES // SLAB, v * LANES % SLAB
                h_ref[side, q, at, c:c + LANES] = (part * sign).astype(jnp.bfloat16)
        return 0

    lax.fori_loop(0, half // LANES, step, 0)


def build_left(left_ref, left):
    def step(j, _):
        bits = left_ref[:, pl.ds(pl.multiple_of(j * HB, HB), HB)]
        left[j] = down((2 * bits - 1).astype(jnp.float32))
        return 0

    lax.fori_loop(0, left.shape[0], step, 0)


def build_order(p_ref):
    size = p_ref.shape[0]
    octets = SLAB // OCT

    def step(s, _):
        lane = iota((size, LANES), 1)
        wanted = lane // octets * SLAB + lane % octets * OCT + s
        hit = (wanted == iota((size, LANES), 0)).astype(jnp.float32)
        p_ref[:, pl.ds(pl.multiple_of(s * LANES, LANES), LANES)] = hit.astype(jnp.bfloat16)
        return 0

    lax.fori_loop(0, OCT, step, 0)


def fold_rows(parts):
    step = 1
    while step < len(parts):
        mixed = list(parts)
        for k in range(len(parts)):
            if not k & step:
                mixed[k] = parts[k] + parts[k + step]
                mixed[k + step] = parts[k] - parts[k + step]
        parts, step = mixed, 2 * step
    return parts


def loop(count, step):
    def run(i, _):
        step(i)
        return 0

    lax.fori_loop(0, count, run, 0)


def kernel(
    peers, experts, x_hbm, left_hbm, right_hbm, group_hbm, near_hbm, gather_hbm, spread_hbm,
    scaled_ref, error_ref, scale_ref, mean_ref, total_ref,
    x_ref, left_ref, right_ref, group_ref, near, gather, spread,
    left, h_ref, p_ref, cols, out_s, in_s, planar_ref, planar_group, peaks, peak_ref, natural_ref, factor_ref,
    sum_ref, sums,
    send1, recv1, send2, recv2, send3, recv3, send_s, recv_s, send4, recv4, load_sem,
):
    blocks, _, width = x_ref.shape
    half = width // 2
    slabs = width // SLAB
    pairs = slabs // 2
    mates = peers // 2
    rows = blocks * SUB
    me = lax.axis_index("row")
    mine = lax.axis_index("expert")
    side = me // mates
    slot = me - side * mates
    hub = mates - 1 + side
    far_hub = mates - side
    is_hub = me == hub
    hub_slot = hub - side * mates
    loads = [
        pltpu.make_async_copy(src, dst, load_sem.at[n])
        for n, (src, dst) in enumerate((
            (right_hbm, right_ref), (left_hbm, left_ref), (x_hbm, x_ref), (group_hbm, group_ref),
            (gather_hbm.at[side], gather), (near_hbm.at[side], near), (spread_hbm.at[side], spread),
        ))
    ]
    for load in loads:
        load.start()
    others = [lax.rem(me + d, peers) for d in range(1, peers)]
    devices = peers * experts
    here = mine * peers + me
    mate_slots = [lax.rem(hub_slot + d, mates) for d in range(1, mates)]

    def who_index(who):
        return jnp.where(who > hub_slot, who - 1, who)

    def remote(src, dst, send_sem, recv_sem, peer):
        return pltpu.make_async_remote_copy(
            src_ref=src, dst_ref=dst, send_sem=send_sem, recv_sem=recv_sem,
            device_id={"row": peer}, device_id_type=MESH,
        )

    def to_hub(s, k, who):
        piece = cols.at[s, k, who]
        return remote(piece, piece, send1.at[s], recv1.at[s, k, who_index(who)], hub)

    def all_to_hub(s):
        piece = cols.at[s, :, slot]
        return remote(piece, piece, send1.at[s], recv1.at[s, 0, 0], hub)

    def from_hub(s, k, who):
        return remote(
            cols.at[s, k, who], cols.at[s, k, hub_slot], send2.at[s, who_index(who)], recv2.at[s, k // PACK],
            side * mates + who,
        )

    def all_from_hub(s, who):
        piece = cols.at[s, :, who]
        return remote(piece, piece, send2.at[s, who_index(who)], recv2.at[s, 0], side * mates + who)

    def four_from_hub(s, kk):
        piece = cols.at[s, pl.ds(kk * PACK, PACK), hub_slot]
        return remote(piece, piece, send2.at[s, 0], recv2.at[s, kk], hub)

    def across(s, k):
        return remote(out_s.at[s, k], in_s.at[s, k], send_s.at[s], recv_s.at[s, k], far_hub)

    def all_across(s):
        return remote(out_s.at[s], in_s.at[s], send_s.at[s], recv_s.at[s, 0], far_hub)

    def share_peak(t, s, peer):
        piece = peaks.at[t, s]
        return remote(piece, piece, send3.at[peer], recv3.at[t, s], peer)

    def all_peaks(peer):
        return remote(peaks.at[side], peaks.at[side], send3.at[peer], recv3.at[0, 0], peer)

    def wrap(value, bound):
        return jnp.where(value >= bound, value - bound, value)

    places = [
        {"expert": wrap(mine + e, experts), "row": wrap(me + r, peers)}
        for e in range(experts) for r in range(peers) if e + r
    ]

    def share_sum(place):
        piece = sums.at[here]
        return pltpu.make_async_remote_copy(
            src_ref=piece, dst_ref=piece, send_sem=send4, recv_sem=recv4, device_id=place, device_id_type=MESH
        )

    def all_sums():
        piece = sums.at[pl.ds(0, devices - 1)]
        return pltpu.make_async_remote_copy(
            src_ref=piece, dst_ref=piece, send_sem=send4, recv_sem=recv4, device_id=places[0], device_id_type=MESH
        )

    barrier = pltpu.get_barrier_semaphore()

    for place in places:
        pl.semaphore_signal(barrier, inc=1, device_id=place, device_id_type=MESH)
    loads[0].wait()
    build_column(right_ref, h_ref, 1.0 / math.sqrt(width * HB))
    loads[1].wait()
    build_left(left_ref, left)
    loads[2].wait()

    def column_side(q):
        def step(j):
            low = jnp.dot(x_ref[j, :, :half], h_ref[0, q], preferred_element_type=jnp.float32)
            high = jnp.dot(x_ref[j, :, half:], h_ref[1, q], preferred_element_type=jnp.float32)
            sign = jnp.concatenate([left[j]] * (SLAB // LANES), axis=1)
            for s, both in ((q, low + high), (q + pairs, low - high)):
                both = both * sign
                parts = fold_rows([both[k * SUB:(k + 1) * SUB] for k in range(FOLD)])
                for k in range(FOLD):
                    cols[s, k, slot, pl.ds(pl.multiple_of(j * SUB, SUB), SUB), :] = parts[k].astype(jnp.bfloat16)

        loop(blocks, step)

    def send_slab(s):
        loop(FOLD, lambda k: to_hub(s, k, slot).start())

    def forward(s, k):
        for who in mate_slots:
            to_hub(s, k, who).wait_recv()
        z = cols[s, k].reshape(mates * rows, SLAB)
        r = jnp.dot(gather[...], z, preferred_element_type=jnp.float32)
        out_s[s, k] = r.astype(jnp.bfloat16)
        across(s, k).start()

    def backward(s, k):
        across(s, k).wait_recv()
        z = cols[s, k].reshape(mates * rows, SLAB)
        r = jnp.dot(near[...], z, preferred_element_type=jnp.float32)
        r = r + jnp.dot(spread[...], in_s[s, k], preferred_element_type=jnp.float32)
        cols[s, k] = r.astype(jnp.bfloat16).reshape(mates, rows, SLAB)
        peak_ref[...] = jnp.maximum(peak_ref[...], jnp.max(jnp.abs(r).reshape(-1, 8, SLAB), axis=0))

        @pl.when(k == FOLD - 1)
        def _():
            peaks[side, s] = jnp.broadcast_to(jnp.max(peak_ref[...], axis=0, keepdims=True), (8, SLAB))
            for peer in others:
                share_peak(side, s, peer).start()

        for who in mate_slots:
            from_hub(s, k, who).start()

    def group_scale(first, count):
        span = count * SLAB
        slab = [jnp.clip(first + i, 0, slabs - 1) for i in range(count)]
        top = jnp.concatenate([jnp.maximum(peaks[0, t], peaks[1, t])[:1] for t in slab], axis=1)
        group = jnp.concatenate(
            [group_ref[:, pl.ds(pl.multiple_of(t * SLAB, SLAB), SLAB)] for t in slab], axis=1
        )
        inside = group == iota((GROUPS, span), 0)
        return jnp.maximum(jnp.max(jnp.where(inside, top, 0.0), axis=1, keepdims=True), 1.0)

    total_rows = peers * blocks * HB
    unroll = next(u for u in (7, 1) if blocks % u == 0)

    def scale_slab(s):
        last = jnp.minimum(s + 1, slabs - 1)

        def peak_in(t):
            @pl.when(jnp.logical_or(jnp.logical_not(is_hub), side != t))
            def _():
                @pl.when(s == 0)
                def _():
                    share_peak(t, 0, me).wait_recv()

                @pl.when(s + 1 < slabs)
                def _():
                    share_peak(t, last, me).wait_recv()

        for t in range(2):
            peak_in(t)
        factor = 2.0 / group_scale(s - 1, 3)
        wide = group_ref[:, pl.ds(pl.multiple_of(s * SLAB, SLAB), SLAB)] == iota((GROUPS, SLAB), 0)
        natural_ref[...] = jnp.max(jnp.where(wide, factor, 0.0), axis=0, keepdims=True)
        wide = planar_group[pl.ds(s, 1), :] == iota((GROUPS, OCT * LANES), 0).astype(jnp.float32)
        factor_ref[...] = jnp.max(jnp.where(wide, factor, 0.0), axis=0, keepdims=True)

    def permute(s, kk):
        @pl.when(jnp.logical_not(is_hub))
        def _():
            four_from_hub(s, kk).wait_recv()

        both = jnp.concatenate([cols[s, kk * PACK + g, hub_slot] for g in range(PACK)], axis=1)
        planar_ref[s % 2, kk] = jnp.dot(both, p_ref[...], preferred_element_type=jnp.float32)

    def lattice(s, kk):
        at_slab = pl.ds(pl.multiple_of(s * SLAB, SLAB), SLAB)
        octets = SLAB // OCT
        lane = iota((SUB, LANES), 1)
        place = s % PACK
        inside = lane // octets == place
        at_error = pl.ds(pl.multiple_of(s // PACK * LANES, LANES), LANES)
        first = (me * (blocks * HB) + (kk * PACK + lane // octets) * SUB + iota((SUB, LANES), 0)).astype(jnp.float32)

        def tile(j):
            at = pl.ds(pl.multiple_of(j * SUB, SUB), SUB)
            natural = natural_ref[...]
            for g in range(PACK):
                value = cols[s, kk * PACK + g, hub_slot, at, :].astype(jnp.float32) * natural
                scaled_ref[j, kk * PACK + g, :, at_slab] = value.astype(jnp.bfloat16)
            square = near_sum = low = size = most = least = None
            for c in range(OCT):
                value = planar_ref[s % 2, kk, at, c * LANES:(c + 1) * LANES] * factor_ref[:, c * LANES:(c + 1) * LANES]
                nearest = jnp.round(value)
                offset = jnp.abs(value - nearest)
                below = jnp.floor(value)
                if c == 0:
                    square, near_sum, low, size = offset * offset, nearest, below, offset
                    most = least = offset
                else:
                    square, near_sum, low = square + offset * offset, near_sum + nearest, low + below
                    size = size + offset
                    most, least = jnp.maximum(most, offset), jnp.minimum(least, offset)
            odd = near_sum - 2.0 * jnp.floor(near_sum * 0.5) > 0.5
            whole = jnp.where(odd, square + (1.0 - 2.0 * most), square)
            shifted = square + (OCT * 0.25 - size)
            odd = low - 2.0 * jnp.floor(low * 0.5) > 0.5
            error = jnp.minimum(whole, jnp.where(odd, shifted + 2.0 * least, shifted))
            for g in range(PACK):
                turned = pltpu.roll(error, lax.rem(place + PACK - g, PACK) * octets, 1)
                old = error_ref[j, kk * PACK + g, :, at_error]
                error_ref[j, kk * PACK + g, :, at_error] = jnp.where(inside, turned, old)
            row = first + (j * HB).astype(jnp.float32)
            return error * ((1.0 + 4.0 * (row + 0.5) / total_rows) / 3.0)

        def some(i):
            parts = [tile(i * unroll + u) for u in range(unroll)]
            sum_ref[...] += sum(parts[1:], parts[0])

        loop(blocks // unroll, some)

    column_side(0)
    pl.semaphore_wait(barrier, devices - 1)

    @pl.when(jnp.logical_not(is_hub))
    def _():
        send_slab(0)

        def step(q):
            column_side(q + 1)
            send_slab(q + 1)

        loop(pairs - 1, step)
        loop(slabs - pairs, lambda q: send_slab(q + pairs))

    for load in loads[3:]:
        load.wait()

    @pl.when(is_hub)
    def _():
        loop(LEAD, lambda k: forward(0, k))

    build_order(p_ref)
    sum_ref[...] = jnp.zeros_like(sum_ref)
    row = jnp.concatenate([group_ref[:, s * SLAB:(s + 1) * SLAB] for s in range(slabs)], axis=0)
    row = jnp.concatenate([row.astype(jnp.float32).astype(jnp.bfloat16)] * PACK, axis=1)
    planar_group[...] = jnp.dot(row, p_ref[...], preferred_element_type=jnp.float32)

    def stage(t):
        mixes = jnp.logical_and(is_hub, t < slabs)

        @pl.when(mixes)
        def _():
            peak_ref[...] = jnp.zeros_like(peak_ref)

        @pl.when(jnp.logical_and(is_hub, t + 1 < pairs))
        def _():
            column_side(t + 1)

        def part(kk):
            @pl.when(mixes)
            def _():
                def step(i):
                    k = kk * PACK + i
                    ahead = t * FOLD + k + LEAD

                    @pl.when(ahead < slabs * FOLD)
                    def _():
                        forward(ahead // FOLD, ahead % FOLD)

                    backward(t, k)

                loop(PACK, step)

            @pl.when(t >= 2)
            def _():
                @pl.when(kk == 0)
                def _():
                    scale_slab(t - 2)

                lattice(t - 2, kk)

            come = jnp.where(is_hub, t, t - kk)

            @pl.when(jnp.logical_and(come >= 0, come < slabs))
            def _():
                permute(come, kk)

        loop(FOLD // PACK, part)

    loop(slabs + 2, stage)

    peak = group_scale(0, slabs) * 0.5
    scale_ref[...] = jnp.broadcast_to(peak, (GROUPS, LANES)).T[:1, :GROUPS]

    part = jnp.sum(jnp.sum(sum_ref[...], axis=0, keepdims=True), axis=1, keepdims=True)
    sums[here] = jnp.broadcast_to(part / (total_rows * width // OCT), (1, LANES))
    for place in places:
        share_sum(place).start()
    all_sums().wait_recv()
    total = jnp.sum(sums[...], axis=0)
    mean = jnp.sum(sums[pl.ds(mine * peers, peers)], axis=0)
    mean_ref[0] = jnp.max(mean)
    total_ref[0] = jnp.max(total / experts)

    @pl.when(jnp.logical_not(is_hub))
    def _():
        loop(slabs, lambda s: all_to_hub(s).wait_send())

    @pl.when(is_hub)
    def _():
        for peer in others:
            all_peaks(peer).wait_send()

        def drain(s):
            all_across(s).wait_send()
            for who in mate_slots:
                all_from_hub(s, who).wait_send()

        loop(slabs, drain)

    all_sums().wait_send()


def put_kernel(scaled_ref, error_ref, scaled_out, error_out, sems):
    copies = (
        pltpu.make_async_copy(scaled_ref, scaled_out, sems.at[0]),
        pltpu.make_async_copy(error_ref, error_out, sems.at[1]),
    )
    for copy in copies:
        copy.start()
    for copy in copies:
        copy.wait()


def put(scaled, errors):
    return pl.pallas_call(
        put_kernel,
        out_shape=(
            jax.ShapeDtypeStruct(scaled.shape, scaled.dtype),
            jax.ShapeDtypeStruct(errors.shape, errors.dtype),
        ),
        in_specs=[pl.BlockSpec(memory_space=pltpu.VMEM)] * 2,
        out_specs=[pl.BlockSpec(memory_space=pl.ANY)] * 2,
        scratch_shapes=[pltpu.SemaphoreType.DMA((2,))],
        compiler_params=pltpu.CompilerParams(vmem_limit_bytes=16 * 2**20),
    )(scaled, errors)


def body(weights, left_bits, right_bits, groups):
    _, local_rows, width = weights.shape
    peers = lax.axis_size("row")
    experts = lax.axis_size("expert")
    blocks = local_rows // HB
    half = width // 2
    mates = peers // 2
    rows = blocks * SUB
    slabs = width // SLAB
    near, gather, spread = row_tables(BLOCKS)
    inner, reach = mates * rows, gather.shape[1]
    vmem = pl.BlockSpec(memory_space=pltpu.VMEM)
    hbm = pl.BlockSpec(memory_space=pl.ANY)
    dma = pltpu.SemaphoreType.DMA
    smem = pl.BlockSpec(memory_space=pltpu.SMEM)
    scaled, errors, group_scale, mean, total = pl.pallas_call(
        functools.partial(kernel, peers, experts),
        out_shape=(
            pltpu.VMEM((blocks, FOLD, SUB, width), jnp.bfloat16),
            pltpu.VMEM((blocks, FOLD, SUB, width // OCT), jnp.float32),
            jax.ShapeDtypeStruct((1, GROUPS), jnp.float32),
            jax.ShapeDtypeStruct((1,), jnp.float32),
            jax.ShapeDtypeStruct((1,), jnp.float32),
        ),
        in_specs=[hbm] * 7,
        out_specs=(vmem, vmem, vmem, smem, smem),
        scratch_shapes=[
            pltpu.VMEM((blocks, HB, width), jnp.bfloat16),
            pltpu.VMEM((1, local_rows), jnp.int32),
            pltpu.VMEM((1, width), jnp.int32),
            pltpu.VMEM((1, width), jnp.int32),
            pltpu.VMEM((inner, inner), jnp.bfloat16),
            pltpu.VMEM((reach, inner), jnp.bfloat16),
            pltpu.VMEM((inner, reach), jnp.bfloat16),
            pltpu.VMEM((blocks, HB, LANES), jnp.float32),
            pltpu.VMEM((2, slabs // 2, half, SLAB), jnp.bfloat16),
            pltpu.VMEM((PACK * SLAB, OCT * LANES), jnp.bfloat16),
            pltpu.VMEM((slabs, FOLD, mates, rows, SLAB), jnp.bfloat16),
            pltpu.VMEM((slabs, FOLD, reach, SLAB), jnp.bfloat16),
            pltpu.VMEM((slabs, FOLD, reach, SLAB), jnp.bfloat16),
            pltpu.VMEM((2, FOLD // PACK, rows, OCT * LANES), jnp.float32),
            pltpu.VMEM((slabs, OCT * LANES), jnp.float32),
            pltpu.VMEM((2, slabs, 8, SLAB), jnp.float32),
            pltpu.VMEM((8, SLAB), jnp.float32),
            pltpu.VMEM((1, SLAB), jnp.float32),
            pltpu.VMEM((1, OCT * LANES), jnp.float32),
            pltpu.VMEM((SUB, LANES), jnp.float32),
            pltpu.VMEM((peers * experts, 1, LANES), jnp.float32),
            dma((slabs,)),
            dma((slabs, FOLD, max(mates - 1, 1))),
            dma((slabs, max(mates - 1, 1))),
            dma((slabs, FOLD // PACK)),
            dma((peers,)),
            dma((2, slabs)),
            dma((slabs,)),
            dma((slabs, FOLD)),
            dma,
            dma,
            dma((7,)),
        ],
        compiler_params=pltpu.CompilerParams(
            collective_id=0, has_side_effects=True, vmem_limit_bytes=54 * 2**20
        ),
    )(weights.reshape(blocks, HB, width), left_bits, right_bits, groups, near, gather, spread)
    scaled, errors = put(scaled, errors)
    return (
        scaled.reshape(1, local_rows, width),
        errors.reshape(1, local_rows, width // OCT),
        group_scale,
        mean,
        total.reshape(()),
    )


def solution(mesh):
    placed = (P("expert", "row", None), P("expert", "row"), P("expert", None), P("expert", None))
    return jax.shard_map(
        body,
        mesh=mesh,
        in_specs=placed,
        out_specs=(
            P("expert", "row", None),
            P("expert", "row", None),
            P("expert", None),
            P("expert"),
            P(),
        ),
        check_vma=False,
    )
```

```python
import functools
import math

import jax
import jax.numpy as jnp
import numpy as np
from jax import lax
from jax.experimental import pallas as pl
from jax.experimental.pallas import tpu as pltpu
from jax.sharding import PartitionSpec as P

HB = 128
SUB = 16
FOLD = HB // SUB
OCT = 8
LANES = 128
GROUPS = 16
BLOCKS = 56
SLAB = 256
PACK = LANES * OCT // SLAB
LEAD = 3
EARLY = 5
MESH = pl.DeviceIdType.MESH


def signs(common, bits):
    for shift in (4, 2, 1):
        if shift < bits:
            common = common ^ (common >> shift)
    return (1 - 2 * (common & 1)).astype(jnp.float32)


def iota(shape, dim):
    return lax.broadcasted_iota(jnp.int32, shape, dim)


def down(row):
    return jnp.broadcast_to(row, (LANES, LANES)).T


def cosine_table(order):
    first = np.arange(order, dtype=np.float64)[:, None]
    second = np.arange(order, dtype=np.float64)[None, :]
    table = math.sqrt(2.0 / order) * np.cos(math.pi * (2.0 * second + 1.0) * first / (2.0 * order))
    return np.where(first == 0.0, table * math.sqrt(0.5), table)


def cross_factors(order, to, own):
    half = order // 2
    block = cosine_table(order)[to * half:(to + 1) * half, (1 - to) * half:(2 - to) * half]
    even, odd = block[0::2], block[1::2]
    along = odd @ even.T / np.sum(even * even, axis=1)
    _, s, v = np.linalg.svd(odd - along @ even)
    kept = int(np.sum(s > 2.0 ** -24))
    basis = np.concatenate([even / np.sqrt(np.sum(even * even, axis=1, keepdims=True)), v[:kept]])
    far = slice(0, half - own) if to else slice(own, half)
    alone = max(0, basis.shape[0] - (half - own))
    if alone:
        turn = np.linalg.svd(basis[:, far].T)[2][::-1]
        basis = turn @ basis
        basis[:alone, far] = 0.0
    return basis, block @ basis.T, alone


def row_tables(order, own):
    half = order // 2
    table = cosine_table(order)
    near = np.stack([table[s * half:(s + 1) * half, s * half:(s + 1) * half] for s in range(2)])
    to_low, to_high = cross_factors(order, 0, own), cross_factors(order, 1, own)
    gather = np.stack([to_high[0], to_low[0]])
    spread = np.stack([to_low[1], to_high[1]])
    index = np.arange(SUB)
    inner = np.array([[1 - 2 * (bin(a & b).count("1") & 1) for b in index] for a in index], np.float32)
    tables = [
        np.stack([np.kron(t, m) for t in ts]).astype(np.float32).astype(np.dtype(jnp.bfloat16))
        for ts, m in ((near, inner), (gather, inner), (spread, np.eye(SUB, dtype=np.float32)))
    ]
    alone = to_high[2] * SUB
    first = np.stack([tables[1][0][:alone, (half - own) * SUB:], tables[1][1][:alone, :own * SUB]])
    return tables, first


def build_column(right_ref, h_ref, scale):
    half = h_ref.shape[2]
    square = (LANES, LANES)
    inner = signs(iota(square, 0) & iota(square, 1), 7)

    def step(u, _):
        at = pl.ds(pl.multiple_of(u * LANES, LANES), LANES)
        for side in range(2):
            bits = right_ref[:, pl.ds(pl.multiple_of(side * half + u * LANES, LANES), LANES)]
            part = inner * down((2 * bits - 1).astype(jnp.float32) * scale)
            for v in range(half // LANES):
                common = u & v
                common = common ^ (common >> 4)
                common = common ^ (common >> 2)
                common = common ^ (common >> 1)
                sign = (1 - 2 * (common & 1)).astype(jnp.float32)
                q, c = v * LANES // SLAB, v * LANES % SLAB
                h_ref[side, q, at, c:c + LANES] = (part * sign).astype(jnp.bfloat16)
        return 0

    lax.fori_loop(0, half // LANES, step, 0)


def build_left(left_ref, left):
    def step(j, _):
        bits = left_ref[:, pl.ds(pl.multiple_of(j * HB, HB), HB)]
        left[j] = down((2 * bits - 1).astype(jnp.float32))
        return 0

    lax.fori_loop(0, left.shape[0], step, 0)


def build_order(p_ref):
    size = p_ref.shape[0]
    octets = SLAB // OCT

    def step(s, _):
        lane = iota((size, LANES), 1)
        wanted = lane // octets * SLAB + lane % octets * OCT + s
        hit = (wanted == iota((size, LANES), 0)).astype(jnp.float32)
        p_ref[:, pl.ds(pl.multiple_of(s * LANES, LANES), LANES)] = hit.astype(jnp.bfloat16)
        return 0

    lax.fori_loop(0, OCT, step, 0)


def fold_rows(parts):
    step = 1
    while step < len(parts):
        mixed = list(parts)
        for k in range(len(parts)):
            if not k & step:
                mixed[k] = parts[k] + parts[k + step]
                mixed[k + step] = parts[k] - parts[k + step]
        parts, step = mixed, 2 * step
    return parts


def loop(count, step):
    def run(i, _):
        step(i)
        return 0

    lax.fori_loop(0, count, run, 0)


def kernel(
    peers, experts, alone, x_hbm, left_hbm, right_hbm, group_hbm, near_hbm, gather_hbm, spread_hbm, first_hbm,
    scaled_ref, error_ref, scale_ref, mean_ref, total_ref,
    x_ref, left_ref, right_ref, group_ref, near, gather, spread, first,
    left, h_ref, p_ref, cols, out_s, in_s, planar_ref, planar_group, peaks, peak_ref, natural_ref, factor_ref,
    sum_ref, sums,
    send1, recv1, send2, recv2, send3, recv3, send_s, recv_s, recv_first, send4, recv4, load_sem,
):
    blocks, _, width = x_ref.shape
    half = width // 2
    slabs = width // SLAB
    pairs = slabs // 2
    mates = peers // 2
    rows = blocks * SUB
    me = lax.axis_index("row")
    mine = lax.axis_index("expert")
    side = me // mates
    slot = me - side * mates
    hub = mates - 1 + side
    far_hub = mates - side
    is_hub = me == hub
    hub_slot = hub - side * mates
    loads = [
        pltpu.make_async_copy(src, dst, load_sem.at[n])
        for n, (src, dst) in enumerate((
            (right_hbm, right_ref), (left_hbm, left_ref), (x_hbm, x_ref), (group_hbm, group_ref),
            (first_hbm.at[side], first), (gather_hbm.at[side], gather), (near_hbm.at[side], near), (spread_hbm.at[side], spread),
        ))
    ]
    for load in loads:
        load.start()
    others = [lax.rem(me + d, peers) for d in range(1, peers)]
    devices = peers * experts
    here = mine * peers + me
    mate_slots = [lax.rem(hub_slot + d, mates) for d in range(1, mates)]

    def who_index(who):
        return jnp.where(who > hub_slot, who - 1, who)

    def remote(src, dst, send_sem, recv_sem, peer):
        return pltpu.make_async_remote_copy(
            src_ref=src, dst_ref=dst, send_sem=send_sem, recv_sem=recv_sem,
            device_id={"row": peer}, device_id_type=MESH,
        )

    def to_hub(s, k, who):
        piece = cols.at[s, k, who]
        return remote(piece, piece, send1.at[s], recv1.at[s, k, who_index(who)], hub)

    def all_to_hub(s):
        piece = cols.at[s, :, slot]
        return remote(piece, piece, send1.at[s], recv1.at[s, 0, 0], hub)

    def from_hub(s, k, who):
        return remote(
            cols.at[s, k, who], cols.at[s, k, hub_slot], send2.at[s, who_index(who)], recv2.at[s, k // PACK],
            side * mates + who,
        )

    def all_from_hub(s, who):
        piece = cols.at[s, :, who]
        return remote(piece, piece, send2.at[s, who_index(who)], recv2.at[s, 0], side * mates + who)

    def four_from_hub(s, kk):
        piece = cols.at[s, pl.ds(kk * PACK, PACK), hub_slot]
        return remote(piece, piece, send2.at[s, 0], recv2.at[s, kk], hub)

    def across(s, k):
        return remote(out_s.at[s, k], in_s.at[s, k], send_s.at[s], recv_s.at[s, k], far_hub)

    def across_part(k, low):
        at = pl.ds(0, alone) if low else pl.ds(alone, gather.shape[0] - alone)
        return remote(
            out_s.at[0, k, at], in_s.at[0, k, at], send_s.at[0],
            recv_first.at[k] if low else recv_s.at[0, k], far_hub,
        )

    def all_across(s):
        return remote(out_s.at[s], in_s.at[s], send_s.at[s], recv_s.at[s, 0], far_hub)

    def share_peak(t, s, peer):
        piece = peaks.at[t, s]
        return remote(piece, piece, send3.at[peer], recv3.at[t, s], peer)

    def all_peaks(peer):
        return remote(peaks.at[side], peaks.at[side], send3.at[peer], recv3.at[0, 0], peer)

    def wrap(value, bound):
        return jnp.where(value >= bound, value - bound, value)

    def each_other(act):
        def step(e):
            for r in range(peers):
                place = {"expert": wrap(mine + e, experts), "row": wrap(me + r, peers)}
                if r:
                    act(place)
                else:
                    pl.when(e > 0)(lambda: act(place))

        loop(experts, step)

    def share_sum(place):
        piece = sums.at[here]
        return pltpu.make_async_remote_copy(
            src_ref=piece, dst_ref=piece, send_sem=send4, recv_sem=recv4, device_id=place, device_id_type=MESH
        )

    def all_sums():
        piece = sums.at[pl.ds(0, devices - 1)]
        return pltpu.make_async_remote_copy(
            src_ref=piece, dst_ref=piece, send_sem=send4, recv_sem=recv4, device_id={"row": others[0]},
            device_id_type=MESH,
        )

    barrier = pltpu.get_barrier_semaphore()

    each_other(lambda place: pl.semaphore_signal(barrier, inc=1, device_id=place, device_id_type=MESH))
    loads[0].wait()
    build_column(right_ref, h_ref, 1.0 / math.sqrt(width * HB))
    loads[1].wait()
    build_left(left_ref, left)
    loads[2].wait()

    def column_side(q):
        def step(j):
            low = jnp.dot(x_ref[j, :, :half], h_ref[0, q], preferred_element_type=jnp.float32)
            high = jnp.dot(x_ref[j, :, half:], h_ref[1, q], preferred_element_type=jnp.float32)
            sign = jnp.concatenate([left[j]] * (SLAB // LANES), axis=1)
            for s, both in ((q, low + high), (q + pairs, low - high)):
                both = both * sign
                parts = fold_rows([both[k * SUB:(k + 1) * SUB] for k in range(FOLD)])
                for k in range(FOLD):
                    cols[s, k, slot, pl.ds(pl.multiple_of(j * SUB, SUB), SUB), :] = parts[k].astype(jnp.bfloat16)

        loop(blocks, step)

    def send_slab(s):
        loop(FOLD, lambda k: to_hub(s, k, slot).start())

    def forward(s, k):
        for who in mate_slots:
            to_hub(s, k, who).wait_recv()

        def full():
            z = cols[s, k].reshape(mates * rows, SLAB)
            r = jnp.dot(gather[...], z, preferred_element_type=jnp.float32)
            out_s[s, k] = r.astype(jnp.bfloat16)
            across(s, k).start()

        def remainder():
            z = cols[0, k].reshape(mates * rows, SLAB)
            r = jnp.dot(gather[alone:, :], z, preferred_element_type=jnp.float32)
            out_s[0, k, alone:, :] = r.astype(jnp.bfloat16)
            across_part(k, False).start()

        if early:
            begun = jnp.logical_and(s == 0, k < early)
            pl.when(begun)(remainder)
            pl.when(jnp.logical_not(begun))(full)
        else:
            full()

    def forward_alone(k):
        r = jnp.dot(first[...], cols[0, k, hub_slot], preferred_element_type=jnp.float32)
        out_s[0, k, :alone, :] = r.astype(jnp.bfloat16)
        across_part(k, True).start()

    def backward(s, k):
        if early:
            begun = jnp.logical_and(s == 0, k < early)

            @pl.when(begun)
            def _():
                across_part(k, True).wait_recv()
                across_part(k, False).wait_recv()

            pl.when(jnp.logical_not(begun))(lambda: across(s, k).wait_recv())
        else:
            across(s, k).wait_recv()
        z = cols[s, k].reshape(mates * rows, SLAB)
        r = jnp.dot(near[...], z, preferred_element_type=jnp.float32)
        r = r + jnp.dot(spread[...], in_s[s, k], preferred_element_type=jnp.float32)
        cols[s, k] = r.astype(jnp.bfloat16).reshape(mates, rows, SLAB)
        peak_ref[...] = jnp.maximum(peak_ref[...], jnp.max(jnp.abs(r).reshape(-1, 8, SLAB), axis=0))

        @pl.when(k == FOLD - 1)
        def _():
            peaks[side, s] = jnp.broadcast_to(jnp.max(peak_ref[...], axis=0, keepdims=True), (8, SLAB))
            for peer in others:
                share_peak(side, s, peer).start()

        for who in mate_slots:
            from_hub(s, k, who).start()

    def group_scale(first, count):
        span = count * SLAB
        slab = [jnp.clip(first + i, 0, slabs - 1) for i in range(count)]
        top = jnp.concatenate([jnp.maximum(peaks[0, t], peaks[1, t])[:1] for t in slab], axis=1)
        group = jnp.concatenate(
            [group_ref[:, pl.ds(pl.multiple_of(t * SLAB, SLAB), SLAB)] for t in slab], axis=1
        )
        inside = group == iota((GROUPS, span), 0)
        return jnp.maximum(jnp.max(jnp.where(inside, top, 0.0), axis=1, keepdims=True), 1.0)

    total_rows = peers * blocks * HB
    early = EARLY if alone else 0
    unroll = next(u for u in (7, 1) if blocks % u == 0)

    def scale_slab(s):
        last = jnp.minimum(s + 1, slabs - 1)

        def peak_in(t):
            @pl.when(jnp.logical_or(jnp.logical_not(is_hub), side != t))
            def _():
                @pl.when(s == 0)
                def _():
                    share_peak(t, 0, me).wait_recv()

                @pl.when(s + 1 < slabs)
                def _():
                    share_peak(t, last, me).wait_recv()

        for t in range(2):
            peak_in(t)
        factor = 2.0 / group_scale(s - 1, 3)
        wide = group_ref[:, pl.ds(pl.multiple_of(s * SLAB, SLAB), SLAB)] == iota((GROUPS, SLAB), 0)
        natural_ref[pl.ds(s % 2, 1), :] = jnp.max(jnp.where(wide, factor, 0.0), axis=0, keepdims=True)
        wide = planar_group[pl.ds(s, 1), :] == iota((GROUPS, OCT * LANES), 0).astype(jnp.float32)
        factor_ref[...] = jnp.max(jnp.where(wide, factor, 0.0), axis=0, keepdims=True)

    def permute(s, kk):
        @pl.when(jnp.logical_not(is_hub))
        def _():
            four_from_hub(s, kk).wait_recv()

        both = jnp.concatenate([cols[s, kk * PACK + g, hub_slot] for g in range(PACK)], axis=1)
        planar_ref[s % 2, kk] = jnp.dot(both, p_ref[...], preferred_element_type=jnp.float32)

    def write_scaled(s, kk):
        at_slab = pl.ds(pl.multiple_of(s * SLAB, SLAB), SLAB)
        natural = natural_ref[pl.ds(s % 2, 1), :]

        def tile(j):
            at = pl.ds(pl.multiple_of(j * SUB, SUB), SUB)
            for g in range(PACK):
                value = cols[s, kk * PACK + g, hub_slot, at, :].astype(jnp.float32) * natural
                scaled_ref[j, kk * PACK + g, :, at_slab] = value.astype(jnp.bfloat16)

        def some(i):
            for u in range(unroll):
                tile(i * unroll + u)

        loop(blocks // unroll, some)

    def lattice(s, kk):
        octets = SLAB // OCT
        lane = iota((SUB, LANES), 1)
        place = s % PACK
        inside = lane // octets == place
        at_error = pl.ds(pl.multiple_of(s // PACK * LANES, LANES), LANES)
        first = (me * (blocks * HB) + (kk * PACK + lane // octets) * SUB + iota((SUB, LANES), 0)).astype(jnp.float32)

        def tile(j):
            at = pl.ds(pl.multiple_of(j * SUB, SUB), SUB)
            square = near_sum = low = size = most = least = None
            for c in range(OCT):
                value = planar_ref[s % 2, kk, at, c * LANES:(c + 1) * LANES] * factor_ref[:, c * LANES:(c + 1) * LANES]
                nearest = jnp.round(value)
                offset = jnp.abs(value - nearest)
                below = jnp.floor(value)
                if c == 0:
                    square, near_sum, low, size = offset * offset, nearest, below, offset
                    most = least = offset
                else:
                    square, near_sum, low = square + offset * offset, near_sum + nearest, low + below
                    size = size + offset
                    most, least = jnp.maximum(most, offset), jnp.minimum(least, offset)
            odd = near_sum - 2.0 * jnp.floor(near_sum * 0.5) > 0.5
            whole = jnp.where(odd, square + (1.0 - 2.0 * most), square)
            shifted = square + (OCT * 0.25 - size)
            odd = low - 2.0 * jnp.floor(low * 0.5) > 0.5
            error = jnp.minimum(whole, jnp.where(odd, shifted + 2.0 * least, shifted))
            for g in range(PACK):
                turned = pltpu.roll(error, lax.rem(place + PACK - g, PACK) * octets, 1)
                old = error_ref[j, kk * PACK + g, :, at_error]
                error_ref[j, kk * PACK + g, :, at_error] = jnp.where(inside, turned, old)
            row = first + (j * HB).astype(jnp.float32)
            return error * ((1.0 + 4.0 * (row + 0.5) / total_rows) / 3.0)

        def some(i):
            parts = [tile(i * unroll + u) for u in range(unroll)]
            sum_ref[...] += sum(parts[1:], parts[0])

        loop(blocks // unroll, some)

    column_side(0)
    pl.semaphore_wait(barrier, devices - 1)

    @pl.when(jnp.logical_not(is_hub))
    def _():
        send_slab(0)

        def step(q):
            column_side(q + 1)
            send_slab(q + 1)

        loop(pairs - 1, step)
        loop(slabs - pairs, lambda q: send_slab(q + pairs))

    for load in loads[3:]:
        load.wait()

    @pl.when(is_hub)
    def _():
        if early:
            loop(early, forward_alone)
        loop(LEAD, lambda k: forward(0, k))

    build_order(p_ref)
    sum_ref[...] = jnp.zeros_like(sum_ref)
    row = jnp.concatenate([group_ref[:, s * SLAB:(s + 1) * SLAB] for s in range(slabs)], axis=0)
    row = jnp.concatenate([row.astype(jnp.float32).astype(jnp.bfloat16)] * PACK, axis=1)
    planar_group[...] = jnp.dot(row, p_ref[...], preferred_element_type=jnp.float32)

    def stage(t):
        mixes = jnp.logical_and(is_hub, t < slabs)

        @pl.when(mixes)
        def _():
            peak_ref[...] = jnp.zeros_like(peak_ref)

        @pl.when(jnp.logical_and(is_hub, t + 1 < pairs))
        def _():
            column_side(t + 1)

        def part(kk):
            @pl.when(mixes)
            def _():
                def step(i):
                    k = kk * PACK + i
                    ahead = t * FOLD + k + LEAD

                    @pl.when(ahead < slabs * FOLD)
                    def _():
                        forward(ahead // FOLD, ahead % FOLD)

                    backward(t, k)

                loop(PACK, step)

            @pl.when(t >= 2)
            def _():
                @pl.when(kk == 0)
                def _():
                    scale_slab(t - 2)

                lattice(t - 2, kk)
                pl.when(t < slabs)(lambda: write_scaled(t - 2, kk))

            come = jnp.where(is_hub, t, t - kk)

            @pl.when(jnp.logical_and(come >= 0, come < slabs))
            def _():
                permute(come, kk)

        loop(FOLD // PACK, part)

    loop(slabs + 2, stage)

    peak = group_scale(0, slabs) * 0.5
    scale_ref[...] = jnp.broadcast_to(peak, (GROUPS, LANES)).T[:1, :GROUPS]

    part = jnp.sum(jnp.sum(sum_ref[...], axis=0, keepdims=True), axis=1, keepdims=True)
    sums[here] = jnp.broadcast_to(part / (total_rows * width // OCT), (1, LANES))
    each_other(lambda place: share_sum(place).start())
    loop(FOLD // PACK, lambda kk: write_scaled(slabs - 2, kk))
    loop(FOLD // PACK, lambda kk: write_scaled(slabs - 1, kk))
    all_sums().wait_recv()
    total = jnp.sum(sums[...], axis=0)
    mean = jnp.sum(sums[pl.ds(mine * peers, peers)], axis=0)
    mean_ref[0] = jnp.max(mean)
    total_ref[0] = jnp.max(total / experts)

    @pl.when(jnp.logical_not(is_hub))
    def _():
        loop(slabs, lambda s: all_to_hub(s).wait_send())

    @pl.when(is_hub)
    def _():
        for peer in others:
            all_peaks(peer).wait_send()

        def drain(s):
            all_across(s).wait_send()
            for who in mate_slots:
                all_from_hub(s, who).wait_send()

        loop(slabs, drain)

    all_sums().wait_send()


def put_kernel(scaled_ref, error_ref, scaled_out, error_out, sems):
    copies = (
        pltpu.make_async_copy(scaled_ref, scaled_out, sems.at[0]),
        pltpu.make_async_copy(error_ref, error_out, sems.at[1]),
    )
    for copy in copies:
        copy.start()
    for copy in copies:
        copy.wait()


def put(scaled, errors):
    return pl.pallas_call(
        put_kernel,
        out_shape=(
            jax.ShapeDtypeStruct(scaled.shape, scaled.dtype),
            jax.ShapeDtypeStruct(errors.shape, errors.dtype),
        ),
        in_specs=[pl.BlockSpec(memory_space=pltpu.VMEM)] * 2,
        out_specs=[pl.BlockSpec(memory_space=pl.ANY)] * 2,
        scratch_shapes=[pltpu.SemaphoreType.DMA((2,))],
        compiler_params=pltpu.CompilerParams(vmem_limit_bytes=16 * 2**20),
    )(scaled, errors)


def body(weights, left_bits, right_bits, groups):
    _, local_rows, width = weights.shape
    peers = lax.axis_size("row")
    experts = lax.axis_size("expert")
    blocks = local_rows // HB
    half = width // 2
    mates = peers // 2
    rows = blocks * SUB
    slabs = width // SLAB
    (near, gather, spread), first = row_tables(BLOCKS, blocks)
    alone = first.shape[1]
    first = first if alone else gather
    inner, reach = mates * rows, gather.shape[1]
    vmem = pl.BlockSpec(memory_space=pltpu.VMEM)
    hbm = pl.BlockSpec(memory_space=pl.ANY)
    dma = pltpu.SemaphoreType.DMA
    smem = pl.BlockSpec(memory_space=pltpu.SMEM)
    scaled, errors, group_scale, mean, total = pl.pallas_call(
        functools.partial(kernel, peers, experts, alone),
        out_shape=(
            pltpu.VMEM((blocks, FOLD, SUB, width), jnp.bfloat16),
            pltpu.VMEM((blocks, FOLD, SUB, width // OCT), jnp.float32),
            jax.ShapeDtypeStruct((1, GROUPS), jnp.float32),
            jax.ShapeDtypeStruct((1,), jnp.float32),
            jax.ShapeDtypeStruct((1,), jnp.float32),
        ),
        in_specs=[hbm] * 8,
        out_specs=(vmem, vmem, vmem, smem, smem),
        scratch_shapes=[
            pltpu.VMEM((blocks, HB, width), jnp.bfloat16),
            pltpu.VMEM((1, local_rows), jnp.int32),
            pltpu.VMEM((1, width), jnp.int32),
            pltpu.VMEM((1, width), jnp.int32),
            pltpu.VMEM((inner, inner), jnp.bfloat16),
            pltpu.VMEM((reach, inner), jnp.bfloat16),
            pltpu.VMEM((inner, reach), jnp.bfloat16),
            pltpu.VMEM(first.shape[1:], jnp.bfloat16),
            pltpu.VMEM((blocks, HB, LANES), jnp.float32),
            pltpu.VMEM((2, slabs // 2, half, SLAB), jnp.bfloat16),
            pltpu.VMEM((PACK * SLAB, OCT * LANES), jnp.bfloat16),
            pltpu.VMEM((slabs, FOLD, mates, rows, SLAB), jnp.bfloat16),
            pltpu.VMEM((slabs, FOLD, reach, SLAB), jnp.bfloat16),
            pltpu.VMEM((slabs, FOLD, reach, SLAB), jnp.bfloat16),
            pltpu.VMEM((2, FOLD // PACK, rows, OCT * LANES), jnp.float32),
            pltpu.VMEM((slabs, OCT * LANES), jnp.float32),
            pltpu.VMEM((2, slabs, 8, SLAB), jnp.float32),
            pltpu.VMEM((8, SLAB), jnp.float32),
            pltpu.VMEM((2, SLAB), jnp.float32),
            pltpu.VMEM((1, OCT * LANES), jnp.float32),
            pltpu.VMEM((SUB, LANES), jnp.float32),
            pltpu.VMEM((peers * experts, 1, LANES), jnp.float32),
            dma((slabs,)),
            dma((slabs, FOLD, max(mates - 1, 1))),
            dma((slabs, max(mates - 1, 1))),
            dma((slabs, FOLD // PACK)),
            dma((peers,)),
            dma((2, slabs)),
            dma((slabs,)),
            dma((slabs, FOLD)),
            dma((EARLY,)),
            dma,
            dma,
            dma((8,)),
        ],
        compiler_params=pltpu.CompilerParams(
            collective_id=0, has_side_effects=True, vmem_limit_bytes=54 * 2**20
        ),
    )(weights.reshape(blocks, HB, width), left_bits, right_bits, groups, near, gather, spread, first)
    scaled, errors = put(scaled, errors)
    return (
        scaled.reshape(1, local_rows, width),
        errors.reshape(1, local_rows, width // OCT),
        group_scale,
        mean,
        total.reshape(()),
    )


def solution(mesh):
    placed = (P("expert", "row", None), P("expert", "row"), P("expert", None), P("expert", None))
    return jax.shard_map(
        body,
        mesh=mesh,
        in_specs=placed,
        out_specs=(
            P("expert", "row", None),
            P("expert", "row", None),
            P("expert", None),
            P("expert"),
            P(),
        ),
        check_vma=False,
    )
```

```python
import functools
import math

import jax
import jax.numpy as jnp
import numpy as np
from jax import lax
from jax.experimental import pallas as pl
from jax.experimental.pallas import tpu as pltpu
from jax.sharding import PartitionSpec as P

HB = 128
SUB = 16
FOLD = HB // SUB
OCT = 8
LANES = 128
GROUPS = 16
BLOCKS = 56
SLAB = 256
PACK = LANES * OCT // SLAB
LEAD = 3
EARLY = 2
MESH = pl.DeviceIdType.MESH


def signs(common, bits):
    for shift in (4, 2, 1):
        if shift < bits:
            common = common ^ (common >> shift)
    return (1 - 2 * (common & 1)).astype(jnp.float32)


def iota(shape, dim):
    return lax.broadcasted_iota(jnp.int32, shape, dim)


def down(row):
    return jnp.broadcast_to(row, (LANES, LANES)).T


def cosine_table(order):
    first = np.arange(order, dtype=np.float64)[:, None]
    second = np.arange(order, dtype=np.float64)[None, :]
    table = math.sqrt(2.0 / order) * np.cos(math.pi * (2.0 * second + 1.0) * first / (2.0 * order))
    return np.where(first == 0.0, table * math.sqrt(0.5), table)


def cross_factors(order, to, own):
    half = order // 2
    block = cosine_table(order)[to * half:(to + 1) * half, (1 - to) * half:(2 - to) * half]
    even, odd = block[0::2], block[1::2]
    along = odd @ even.T / np.sum(even * even, axis=1)
    _, s, v = np.linalg.svd(odd - along @ even)
    kept = int(np.sum(s > 2.0 ** -24))
    basis = np.concatenate([even / np.sqrt(np.sum(even * even, axis=1, keepdims=True)), v[:kept]])
    far = slice(0, half - own) if to else slice(own, half)
    alone = max(0, basis.shape[0] - (half - own))
    if alone:
        turn = np.linalg.svd(basis[:, far].T)[2][::-1]
        basis = turn @ basis
        basis[:alone, far] = 0.0
    return basis, block @ basis.T, alone


def row_tables(order, own):
    half = order // 2
    table = cosine_table(order)
    near = np.stack([table[s * half:(s + 1) * half, s * half:(s + 1) * half] for s in range(2)])
    to_low, to_high = cross_factors(order, 0, own), cross_factors(order, 1, own)
    gather = np.stack([to_high[0], to_low[0]])
    spread = np.stack([to_low[1], to_high[1]])
    index = np.arange(SUB)
    inner = np.array([[1 - 2 * (bin(a & b).count("1") & 1) for b in index] for a in index], np.float32)
    tables = [
        np.stack([np.kron(t, m) for t in ts]).astype(np.float32).astype(np.dtype(jnp.bfloat16))
        for ts, m in ((near, inner), (gather, inner), (spread, np.eye(SUB, dtype=np.float32)))
    ]
    alone = to_high[2] * SUB
    first = np.stack([tables[1][0][:alone, (half - own) * SUB:], tables[1][1][:alone, :own * SUB]])
    return tables, first


def build_column(right_ref, h_ref, scale):
    half = h_ref.shape[2]
    square = (LANES, LANES)
    inner = signs(iota(square, 0) & iota(square, 1), 7)

    def step(u, _):
        at = pl.ds(pl.multiple_of(u * LANES, LANES), LANES)
        for side in range(2):
            bits = right_ref[:, pl.ds(pl.multiple_of(side * half + u * LANES, LANES), LANES)]
            part = inner * down((2 * bits - 1).astype(jnp.float32) * scale)
            for v in range(half // LANES):
                common = u & v
                common = common ^ (common >> 4)
                common = common ^ (common >> 2)
                common = common ^ (common >> 1)
                sign = (1 - 2 * (common & 1)).astype(jnp.float32)
                q, c = v * LANES // SLAB, v * LANES % SLAB
                h_ref[side, q, at, c:c + LANES] = (part * sign).astype(jnp.bfloat16)
        return 0

    lax.fori_loop(0, half // LANES, step, 0)


def build_left(left_ref, left):
    def step(j, _):
        bits = left_ref[:, pl.ds(pl.multiple_of(j * HB, HB), HB)]
        left[j] = down((2 * bits - 1).astype(jnp.float32))
        return 0

    lax.fori_loop(0, left.shape[0], step, 0)


def build_order(p_ref):
    size = p_ref.shape[0]
    octets = SLAB // OCT

    def step(s, _):
        lane = iota((size, LANES), 1)
        wanted = lane // octets * SLAB + lane % octets * OCT + s
        hit = (wanted == iota((size, LANES), 0)).astype(jnp.float32)
        p_ref[:, pl.ds(pl.multiple_of(s * LANES, LANES), LANES)] = hit.astype(jnp.bfloat16)
        return 0

    lax.fori_loop(0, OCT, step, 0)


def fold_rows(parts):
    step = 1
    while step < len(parts):
        mixed = list(parts)
        for k in range(len(parts)):
            if not k & step:
                mixed[k] = parts[k] + parts[k + step]
                mixed[k + step] = parts[k] - parts[k + step]
        parts, step = mixed, 2 * step
    return parts


def loop(count, step):
    def run(i, _):
        step(i)
        return 0

    lax.fori_loop(0, count, run, 0)


def kernel(
    peers, experts, alone, x_hbm, left_hbm, right_hbm, group_hbm, near_hbm, gather_hbm, spread_hbm, first_hbm,
    scaled_ref, error_ref, scale_ref, mean_ref, total_ref,
    x_ref, left_ref, right_ref, group_ref, near, gather, spread, first,
    left, h_ref, p_ref, cols, out_s, in_s, planar_ref, planar_group, peaks, peak_ref, natural_ref, factor_ref,
    sum_ref, sums,
    send1, recv1, send2, recv2, send3, recv3, send_s, recv_s, recv_first, send4, recv4, load_sem,
):
    blocks, _, width = x_ref.shape
    half = width // 2
    slabs = width // SLAB
    pairs = slabs // 2
    mates = peers // 2
    rows = blocks * SUB
    me = lax.axis_index("row")
    mine = lax.axis_index("expert")
    side = me // mates
    slot = me - side * mates
    hub = mates - 1 + side
    far_hub = mates - side
    is_hub = me == hub
    hub_slot = hub - side * mates
    loads = [
        pltpu.make_async_copy(src, dst, load_sem.at[n])
        for n, (src, dst) in enumerate((
            (right_hbm, right_ref), (left_hbm, left_ref), (x_hbm, x_ref), (group_hbm, group_ref),
            (first_hbm.at[side], first), (gather_hbm.at[side], gather), (near_hbm.at[side], near), (spread_hbm.at[side], spread),
        ))
    ]
    for load in loads:
        load.start()
    others = [lax.rem(me + d, peers) for d in range(1, peers)]
    devices = peers * experts
    here = mine * peers + me
    mate_slots = [lax.rem(hub_slot + d, mates) for d in range(1, mates)]

    def who_index(who):
        return jnp.where(who > hub_slot, who - 1, who)

    def remote(src, dst, send_sem, recv_sem, peer):
        return pltpu.make_async_remote_copy(
            src_ref=src, dst_ref=dst, send_sem=send_sem, recv_sem=recv_sem,
            device_id={"row": peer}, device_id_type=MESH,
        )

    def to_hub(s, k, who):
        piece = cols.at[s, k, who]
        return remote(piece, piece, send1.at[s], recv1.at[s, k, who_index(who)], hub)

    def all_to_hub(s):
        piece = cols.at[s, :, slot]
        return remote(piece, piece, send1.at[s], recv1.at[s, 0, 0], hub)

    def from_hub(s, k, who):
        return remote(
            cols.at[s, k, who], cols.at[s, k, hub_slot], send2.at[s, who_index(who)], recv2.at[s, k // PACK],
            side * mates + who,
        )

    def all_from_hub(s, who):
        piece = cols.at[s, :, who]
        return remote(piece, piece, send2.at[s, who_index(who)], recv2.at[s, 0], side * mates + who)

    def four_from_hub(s, kk):
        piece = cols.at[s, pl.ds(kk * PACK, PACK), hub_slot]
        return remote(piece, piece, send2.at[s, 0], recv2.at[s, kk], hub)

    def across(s, k):
        return remote(out_s.at[s, k], in_s.at[s, k], send_s.at[s], recv_s.at[s, k], far_hub)

    def across_part(s, k, low):
        at = pl.ds(0, alone) if low else pl.ds(alone, gather.shape[0] - alone)
        return remote(
            out_s.at[s, k, at], in_s.at[s, k, at], send_s.at[s],
            recv_first.at[s, k] if low else recv_s.at[s, k], far_hub,
        )

    def all_across(s):
        return remote(out_s.at[s], in_s.at[s], send_s.at[s], recv_s.at[s, 0], far_hub)

    def share_peak(t, s, peer):
        piece = peaks.at[t, s]
        return remote(piece, piece, send3.at[peer], recv3.at[t, s], peer)

    def all_peaks(peer):
        return remote(peaks.at[side], peaks.at[side], send3.at[peer], recv3.at[0, 0], peer)

    def wrap(value, bound):
        return jnp.where(value >= bound, value - bound, value)

    def each_other(act):
        def step(e):
            for r in range(peers):
                place = {"expert": wrap(mine + e, experts), "row": wrap(me + r, peers)}
                if r:
                    act(place)
                else:
                    pl.when(e > 0)(lambda: act(place))

        loop(experts, step)

    def share_sum(place):
        piece = sums.at[here]
        return pltpu.make_async_remote_copy(
            src_ref=piece, dst_ref=piece, send_sem=send4, recv_sem=recv4, device_id=place, device_id_type=MESH
        )

    def all_sums():
        piece = sums.at[pl.ds(0, devices - 1)]
        return pltpu.make_async_remote_copy(
            src_ref=piece, dst_ref=piece, send_sem=send4, recv_sem=recv4, device_id={"row": others[0]},
            device_id_type=MESH,
        )

    barrier = pltpu.get_barrier_semaphore()

    each_other(lambda place: pl.semaphore_signal(barrier, inc=1, device_id=place, device_id_type=MESH))
    loads[0].wait()
    build_column(right_ref, h_ref, 1.0 / math.sqrt(width * HB))
    loads[1].wait()
    build_left(left_ref, left)
    loads[2].wait()

    def column_side(q):
        def step(j):
            low = jnp.dot(x_ref[j, :, :half], h_ref[0, q], preferred_element_type=jnp.float32)
            high = jnp.dot(x_ref[j, :, half:], h_ref[1, q], preferred_element_type=jnp.float32)
            sign = jnp.concatenate([left[j]] * (SLAB // LANES), axis=1)
            for s, both in ((q, low + high), (q + pairs, low - high)):
                both = both * sign
                parts = fold_rows([both[k * SUB:(k + 1) * SUB] for k in range(FOLD)])
                for k in range(FOLD):
                    cols[s, k, slot, pl.ds(pl.multiple_of(j * SUB, SUB), SUB), :] = parts[k].astype(jnp.bfloat16)

        loop(blocks, step)

    def send_slab(s):
        loop(FOLD, lambda k: to_hub(s, k, slot).start())

    def forward(s, k):
        for who in mate_slots:
            to_hub(s, k, who).wait_recv()

        def full():
            z = cols[s, k].reshape(mates * rows, SLAB)
            r = jnp.dot(gather[...], z, preferred_element_type=jnp.float32)
            out_s[s, k] = r.astype(jnp.bfloat16)
            across(s, k).start()

        def remainder():
            z = cols[s, k].reshape(mates * rows, SLAB)
            r = jnp.dot(gather[alone:, :], z, preferred_element_type=jnp.float32)
            out_s[s, k, alone:, :] = r.astype(jnp.bfloat16)
            across_part(s, k, False).start()

        if early:
            pl.when(s < early)(remainder)
            pl.when(s >= early)(full)
        else:
            full()

    def forward_alone(s, k):
        r = jnp.dot(first[...], cols[s, k, hub_slot], preferred_element_type=jnp.float32)
        out_s[s, k, :alone, :] = r.astype(jnp.bfloat16)
        across_part(s, k, True).start()

    def backward(s, k):
        if early:
            @pl.when(s < early)
            def _():
                across_part(s, k, True).wait_recv()
                across_part(s, k, False).wait_recv()

            pl.when(s >= early)(lambda: across(s, k).wait_recv())
        else:
            across(s, k).wait_recv()
        z = cols[s, k].reshape(mates * rows, SLAB)
        r = jnp.dot(near[...], z, preferred_element_type=jnp.float32)
        r = r + jnp.dot(spread[...], in_s[s, k], preferred_element_type=jnp.float32)
        cols[s, k] = r.astype(jnp.bfloat16).reshape(mates, rows, SLAB)
        peak_ref[...] = jnp.maximum(peak_ref[...], jnp.max(jnp.abs(r).reshape(-1, 8, SLAB), axis=0))

        @pl.when(k == FOLD - 1)
        def _():
            peaks[side, s] = jnp.broadcast_to(jnp.max(peak_ref[...], axis=0, keepdims=True), (8, SLAB))
            for peer in others:
                share_peak(side, s, peer).start()

        for who in mate_slots:
            from_hub(s, k, who).start()

    def group_scale(first, count):
        span = count * SLAB
        slab = [jnp.clip(first + i, 0, slabs - 1) for i in range(count)]
        top = jnp.concatenate([jnp.maximum(peaks[0, t], peaks[1, t])[:1] for t in slab], axis=1)
        group = jnp.concatenate(
            [group_ref[:, pl.ds(pl.multiple_of(t * SLAB, SLAB), SLAB)] for t in slab], axis=1
        )
        inside = group == iota((GROUPS, span), 0)
        return jnp.maximum(jnp.max(jnp.where(inside, top, 0.0), axis=1, keepdims=True), 1.0)

    total_rows = peers * blocks * HB
    early = EARLY if alone else 0
    unroll = next(u for u in (7, 1) if blocks % u == 0)

    def scale_slab(s):
        last = jnp.minimum(s + 1, slabs - 1)

        def peak_in(t):
            @pl.when(jnp.logical_or(jnp.logical_not(is_hub), side != t))
            def _():
                @pl.when(s == 0)
                def _():
                    share_peak(t, 0, me).wait_recv()

                @pl.when(s + 1 < slabs)
                def _():
                    share_peak(t, last, me).wait_recv()

        for t in range(2):
            peak_in(t)
        factor = 2.0 / group_scale(s - 1, 3)
        wide = group_ref[:, pl.ds(pl.multiple_of(s * SLAB, SLAB), SLAB)] == iota((GROUPS, SLAB), 0)
        natural_ref[pl.ds(s % 2, 1), :] = jnp.max(jnp.where(wide, factor, 0.0), axis=0, keepdims=True)
        wide = planar_group[pl.ds(s, 1), :] == iota((GROUPS, OCT * LANES), 0).astype(jnp.float32)
        factor_ref[...] = jnp.max(jnp.where(wide, factor, 0.0), axis=0, keepdims=True)

    def permute(s, kk):
        @pl.when(jnp.logical_not(is_hub))
        def _():
            four_from_hub(s, kk).wait_recv()

        both = jnp.concatenate([cols[s, kk * PACK + g, hub_slot] for g in range(PACK)], axis=1)
        planar_ref[s % 2, kk] = jnp.dot(both, p_ref[...], preferred_element_type=jnp.float32)

    def write_scaled(s, kk):
        at_slab = pl.ds(pl.multiple_of(s * SLAB, SLAB), SLAB)
        natural = natural_ref[pl.ds(s % 2, 1), :]

        def tile(j):
            at = pl.ds(pl.multiple_of(j * SUB, SUB), SUB)
            for g in range(PACK):
                value = cols[s, kk * PACK + g, hub_slot, at, :].astype(jnp.float32) * natural
                scaled_ref[j, kk * PACK + g, :, at_slab] = value.astype(jnp.bfloat16)

        def some(i):
            for u in range(unroll):
                tile(i * unroll + u)

        loop(blocks // unroll, some)

    def lattice(s, kk):
        octets = SLAB // OCT
        lane = iota((SUB, LANES), 1)
        place = s % PACK
        inside = lane // octets == place
        at_error = pl.ds(pl.multiple_of(s // PACK * LANES, LANES), LANES)
        first = (me * (blocks * HB) + (kk * PACK + lane // octets) * SUB + iota((SUB, LANES), 0)).astype(jnp.float32)

        def tile(j):
            at = pl.ds(pl.multiple_of(j * SUB, SUB), SUB)
            square = near_sum = low = size = most = least = None
            for c in range(OCT):
                value = planar_ref[s % 2, kk, at, c * LANES:(c + 1) * LANES] * factor_ref[:, c * LANES:(c + 1) * LANES]
                nearest = jnp.round(value)
                offset = jnp.abs(value - nearest)
                below = jnp.floor(value)
                if c == 0:
                    square, near_sum, low, size = offset * offset, nearest, below, offset
                    most = least = offset
                else:
                    square, near_sum, low = square + offset * offset, near_sum + nearest, low + below
                    size = size + offset
                    most, least = jnp.maximum(most, offset), jnp.minimum(least, offset)
            odd = near_sum - 2.0 * jnp.floor(near_sum * 0.5) > 0.5
            whole = jnp.where(odd, square + (1.0 - 2.0 * most), square)
            shifted = square + (OCT * 0.25 - size)
            odd = low - 2.0 * jnp.floor(low * 0.5) > 0.5
            error = jnp.minimum(whole, jnp.where(odd, shifted + 2.0 * least, shifted))
            for g in range(PACK):
                turned = pltpu.roll(error, lax.rem(place + PACK - g, PACK) * octets, 1)
                old = error_ref[j, kk * PACK + g, :, at_error]
                error_ref[j, kk * PACK + g, :, at_error] = jnp.where(inside, turned, old)
            row = first + (j * HB).astype(jnp.float32)
            return error * ((1.0 + 4.0 * (row + 0.5) / total_rows) / 3.0)

        def some(i):
            parts = [tile(i * unroll + u) for u in range(unroll)]
            sum_ref[...] += sum(parts[1:], parts[0])

        loop(blocks // unroll, some)

    column_side(0)
    pl.semaphore_wait(barrier, devices - 1)

    @pl.when(jnp.logical_not(is_hub))
    def _():
        send_slab(0)

        def step(q):
            column_side(q + 1)
            send_slab(q + 1)

        loop(pairs - 1, step)
        loop(slabs - pairs, lambda q: send_slab(q + pairs))

    for load in loads[3:]:
        load.wait()

    @pl.when(is_hub)
    def _():
        def begin(s):
            pl.when(s > 0)(lambda: column_side(s))
            if early:
                loop(FOLD, lambda k: forward_alone(s, k))

        loop(EARLY, begin)
        loop(LEAD, lambda k: forward(0, k))

    build_order(p_ref)
    sum_ref[...] = jnp.zeros_like(sum_ref)
    row = jnp.concatenate([group_ref[:, s * SLAB:(s + 1) * SLAB] for s in range(slabs)], axis=0)
    row = jnp.concatenate([row.astype(jnp.float32).astype(jnp.bfloat16)] * PACK, axis=1)
    planar_group[...] = jnp.dot(row, p_ref[...], preferred_element_type=jnp.float32)

    def stage(t):
        mixes = jnp.logical_and(is_hub, t < slabs)

        @pl.when(mixes)
        def _():
            peak_ref[...] = jnp.zeros_like(peak_ref)

        @pl.when(jnp.logical_and(is_hub, jnp.logical_and(t + 1 >= EARLY, t + 1 < pairs)))
        def _():
            column_side(t + 1)

        def part(kk):
            @pl.when(mixes)
            def _():
                def step(i):
                    k = kk * PACK + i
                    ahead = t * FOLD + k + LEAD

                    @pl.when(ahead < slabs * FOLD)
                    def _():
                        forward(ahead // FOLD, ahead % FOLD)

                    backward(t, k)

                loop(PACK, step)

            @pl.when(t >= 2)
            def _():
                @pl.when(kk == 0)
                def _():
                    scale_slab(t - 2)

                lattice(t - 2, kk)
                pl.when(t < slabs)(lambda: write_scaled(t - 2, kk))

            come = jnp.where(is_hub, t, t - kk)

            @pl.when(jnp.logical_and(come >= 0, come < slabs))
            def _():
                permute(come, kk)

        loop(FOLD // PACK, part)

    loop(slabs + 2, stage)


    part = jnp.sum(jnp.sum(sum_ref[...], axis=0, keepdims=True), axis=1, keepdims=True)
    sums[here] = jnp.broadcast_to(part / (total_rows * width // OCT), (1, LANES))
    each_other(lambda place: share_sum(place).start())
    loop(FOLD // PACK, lambda kk: write_scaled(slabs - 2, kk))
    loop(FOLD // PACK, lambda kk: write_scaled(slabs - 1, kk))
    peak = group_scale(0, slabs) * 0.5
    scale_ref[...] = jnp.broadcast_to(peak, (GROUPS, LANES)).T[:1, :GROUPS]

    @pl.when(jnp.logical_not(is_hub))
    def _():
        loop(slabs, lambda s: all_to_hub(s).wait_send())

    @pl.when(is_hub)
    def _():
        for peer in others:
            all_peaks(peer).wait_send()

        def drain(s):
            all_across(s).wait_send()
            for who in mate_slots:
                all_from_hub(s, who).wait_send()

        loop(slabs, drain)

    all_sums().wait_recv()
    total = jnp.sum(sums[...], axis=0)
    mean = jnp.sum(sums[pl.ds(mine * peers, peers)], axis=0)
    mean_ref[0] = jnp.max(mean)
    total_ref[0] = jnp.max(total / experts)

    all_sums().wait_send()


def put_kernel(scaled_ref, error_ref, scaled_out, error_out, sems):
    copies = (
        pltpu.make_async_copy(scaled_ref, scaled_out, sems.at[0]),
        pltpu.make_async_copy(error_ref, error_out, sems.at[1]),
    )
    for copy in copies:
        copy.start()
    for copy in copies:
        copy.wait()


def put(scaled, errors):
    return pl.pallas_call(
        put_kernel,
        out_shape=(
            jax.ShapeDtypeStruct(scaled.shape, scaled.dtype),
            jax.ShapeDtypeStruct(errors.shape, errors.dtype),
        ),
        in_specs=[pl.BlockSpec(memory_space=pltpu.VMEM)] * 2,
        out_specs=[pl.BlockSpec(memory_space=pl.ANY)] * 2,
        scratch_shapes=[pltpu.SemaphoreType.DMA((2,))],
        compiler_params=pltpu.CompilerParams(vmem_limit_bytes=16 * 2**20),
    )(scaled, errors)


def body(weights, left_bits, right_bits, groups):
    _, local_rows, width = weights.shape
    peers = lax.axis_size("row")
    experts = lax.axis_size("expert")
    blocks = local_rows // HB
    half = width // 2
    mates = peers // 2
    rows = blocks * SUB
    slabs = width // SLAB
    (near, gather, spread), first = row_tables(BLOCKS, blocks)
    alone = first.shape[1]
    first = first if alone else gather
    inner, reach = mates * rows, gather.shape[1]
    vmem = pl.BlockSpec(memory_space=pltpu.VMEM)
    hbm = pl.BlockSpec(memory_space=pl.ANY)
    dma = pltpu.SemaphoreType.DMA
    smem = pl.BlockSpec(memory_space=pltpu.SMEM)
    scaled, errors, group_scale, mean, total = pl.pallas_call(
        functools.partial(kernel, peers, experts, alone),
        out_shape=(
            pltpu.VMEM((blocks, FOLD, SUB, width), jnp.bfloat16),
            pltpu.VMEM((blocks, FOLD, SUB, width // OCT), jnp.float32),
            jax.ShapeDtypeStruct((1, GROUPS), jnp.float32),
            jax.ShapeDtypeStruct((1,), jnp.float32),
            jax.ShapeDtypeStruct((1,), jnp.float32),
        ),
        in_specs=[hbm] * 8,
        out_specs=(vmem, vmem, vmem, smem, smem),
        scratch_shapes=[
            pltpu.VMEM((blocks, HB, width), jnp.bfloat16),
            pltpu.VMEM((1, local_rows), jnp.int32),
            pltpu.VMEM((1, width), jnp.int32),
            pltpu.VMEM((1, width), jnp.int32),
            pltpu.VMEM((inner, inner), jnp.bfloat16),
            pltpu.VMEM((reach, inner), jnp.bfloat16),
            pltpu.VMEM((inner, reach), jnp.bfloat16),
            pltpu.VMEM(first.shape[1:], jnp.bfloat16),
            pltpu.VMEM((blocks, HB, LANES), jnp.float32),
            pltpu.VMEM((2, slabs // 2, half, SLAB), jnp.bfloat16),
            pltpu.VMEM((PACK * SLAB, OCT * LANES), jnp.bfloat16),
            pltpu.VMEM((slabs, FOLD, mates, rows, SLAB), jnp.bfloat16),
            pltpu.VMEM((slabs, FOLD, reach, SLAB), jnp.bfloat16),
            pltpu.VMEM((slabs, FOLD, reach, SLAB), jnp.bfloat16),
            pltpu.VMEM((2, FOLD // PACK, rows, OCT * LANES), jnp.float32),
            pltpu.VMEM((slabs, OCT * LANES), jnp.float32),
            pltpu.VMEM((2, slabs, 8, SLAB), jnp.float32),
            pltpu.VMEM((8, SLAB), jnp.float32),
            pltpu.VMEM((2, SLAB), jnp.float32),
            pltpu.VMEM((1, OCT * LANES), jnp.float32),
            pltpu.VMEM((SUB, LANES), jnp.float32),
            pltpu.VMEM((peers * experts, 1, LANES), jnp.float32),
            dma((slabs,)),
            dma((slabs, FOLD, max(mates - 1, 1))),
            dma((slabs, max(mates - 1, 1))),
            dma((slabs, FOLD // PACK)),
            dma((peers,)),
            dma((2, slabs)),
            dma((slabs,)),
            dma((slabs, FOLD)),
            dma((EARLY, FOLD)),
            dma,
            dma,
            dma((8,)),
        ],
        compiler_params=pltpu.CompilerParams(
            collective_id=0, has_side_effects=True, vmem_limit_bytes=54 * 2**20
        ),
    )(weights.reshape(blocks, HB, width), left_bits, right_bits, groups, near, gather, spread, first)
    scaled, errors = put(scaled, errors)
    return (
        scaled.reshape(1, local_rows, width),
        errors.reshape(1, local_rows, width // OCT),
        group_scale,
        mean,
        total.reshape(()),
    )


def solution(mesh):
    placed = (P("expert", "row", None), P("expert", "row"), P("expert", None), P("expert", None))
    return jax.shard_map(
        body,
        mesh=mesh,
        in_specs=placed,
        out_specs=(
            P("expert", "row", None),
            P("expert", "row", None),
            P("expert", None),
            P("expert"),
            P(),
        ),
        check_vma=False,
    )
```

```python
import functools
import math

import jax
import jax.numpy as jnp
import numpy as np
from jax import lax
from jax.experimental import pallas as pl
from jax.experimental.pallas import tpu as pltpu
from jax.sharding import PartitionSpec as P

HB = 128
SUB = 16
FOLD = HB // SUB
OCT = 8
LANES = 128
GROUPS = 16
BLOCKS = 56
SLAB = 256
PACK = LANES * OCT // SLAB
LEAD = 3
EARLY = 2
MESH = pl.DeviceIdType.MESH


def signs(common, bits):
    for shift in (4, 2, 1):
        if shift < bits:
            common = common ^ (common >> shift)
    return (1 - 2 * (common & 1)).astype(jnp.float32)


def iota(shape, dim):
    return lax.broadcasted_iota(jnp.int32, shape, dim)


def down(row):
    return jnp.broadcast_to(row, (LANES, LANES)).T


def cosine_table(order):
    first = np.arange(order, dtype=np.float64)[:, None]
    second = np.arange(order, dtype=np.float64)[None, :]
    table = math.sqrt(2.0 / order) * np.cos(math.pi * (2.0 * second + 1.0) * first / (2.0 * order))
    return np.where(first == 0.0, table * math.sqrt(0.5), table)


def cross_factors(order, to, own):
    half = order // 2
    block = cosine_table(order)[to * half:(to + 1) * half, (1 - to) * half:(2 - to) * half]
    even, odd = block[0::2], block[1::2]
    along = odd @ even.T / np.sum(even * even, axis=1)
    _, s, v = np.linalg.svd(odd - along @ even)
    kept = int(np.sum(s > 2.0 ** -24))
    basis = np.concatenate([even / np.sqrt(np.sum(even * even, axis=1, keepdims=True)), v[:kept]])
    far = slice(0, half - own) if to else slice(own, half)
    alone = max(0, basis.shape[0] - (half - own))
    if alone:
        turn = np.linalg.svd(basis[:, far].T)[2][::-1]
        basis = turn @ basis
        basis[:alone, far] = 0.0
    return basis, block @ basis.T, alone


def row_tables(order, own):
    half = order // 2
    table = cosine_table(order)
    near = np.stack([table[s * half:(s + 1) * half, s * half:(s + 1) * half] for s in range(2)])
    to_low, to_high = cross_factors(order, 0, own), cross_factors(order, 1, own)
    gather = np.stack([to_high[0], to_low[0]])
    spread = np.stack([to_low[1], to_high[1]])
    index = np.arange(SUB)
    inner = np.array([[1 - 2 * (bin(a & b).count("1") & 1) for b in index] for a in index], np.float32)
    tables = [
        np.stack([np.kron(t, m) for t in ts]).astype(np.float32).astype(np.dtype(jnp.bfloat16))
        for ts, m in ((near, inner), (gather, inner), (spread, np.eye(SUB, dtype=np.float32)))
    ]
    alone = to_high[2] * SUB
    first = np.stack([tables[1][0][:alone, (half - own) * SUB:], tables[1][1][:alone, :own * SUB]])
    return tables, first


def build_column(right_ref, h_ref, scale):
    half = h_ref.shape[2]
    square = (LANES, LANES)
    inner = signs(iota(square, 0) & iota(square, 1), 7)

    def step(u, _):
        at = pl.ds(pl.multiple_of(u * LANES, LANES), LANES)
        for side in range(2):
            bits = right_ref[:, pl.ds(pl.multiple_of(side * half + u * LANES, LANES), LANES)]
            part = inner * down((2 * bits - 1).astype(jnp.float32) * scale)
            for v in range(half // LANES):
                common = u & v
                common = common ^ (common >> 4)
                common = common ^ (common >> 2)
                common = common ^ (common >> 1)
                sign = (1 - 2 * (common & 1)).astype(jnp.float32)
                q, c = v * LANES // SLAB, v * LANES % SLAB
                h_ref[side, q, at, c:c + LANES] = (part * sign).astype(jnp.bfloat16)
        return 0

    lax.fori_loop(0, half // LANES, step, 0)


def build_left(left_ref, left):
    def step(j, _):
        bits = left_ref[:, pl.ds(pl.multiple_of(j * HB, HB), HB)]
        left[j] = down((2 * bits - 1).astype(jnp.float32))
        return 0

    lax.fori_loop(0, left.shape[0], step, 0)


def build_order(p_ref):
    size = p_ref.shape[0]
    octets = SLAB // OCT

    def step(s, _):
        lane = iota((size, LANES), 1)
        wanted = lane // octets * SLAB + lane % octets * OCT + s
        hit = (wanted == iota((size, LANES), 0)).astype(jnp.float32)
        p_ref[:, pl.ds(pl.multiple_of(s * LANES, LANES), LANES)] = hit.astype(jnp.bfloat16)
        return 0

    lax.fori_loop(0, OCT, step, 0)


def fold_rows(parts):
    step = 1
    while step < len(parts):
        mixed = list(parts)
        for k in range(len(parts)):
            if not k & step:
                mixed[k] = parts[k] + parts[k + step]
                mixed[k + step] = parts[k] - parts[k + step]
        parts, step = mixed, 2 * step
    return parts


def loop(count, step):
    def run(i, _):
        step(i)
        return 0

    lax.fori_loop(0, count, run, 0)


def kernel(
    peers, experts, alone, x_hbm, left_hbm, right_hbm, group_hbm, near_hbm, gather_hbm, spread_hbm, first_hbm,
    scaled_ref, error_ref, scale_ref, mean_ref, total_ref,
    x_ref, left_ref, right_ref, group_ref, near, gather, spread, first,
    left, h_ref, p_ref, cols, out_s, in_s, planar_ref, planar_group, peaks, peak_ref, natural_ref, factor_ref,
    sum_ref, sums,
    send1, recv1, send2, recv2, send3, recv3, send_s, recv_s, recv_first, send4, recv4, load_sem,
):
    blocks, _, width = x_ref.shape
    half = width // 2
    slabs = width // SLAB
    pairs = slabs // 2
    mates = peers // 2
    rows = blocks * SUB
    me = lax.axis_index("row")
    mine = lax.axis_index("expert")
    side = me // mates
    slot = me - side * mates
    hub = mates - 1 + side
    far_hub = mates - side
    is_hub = me == hub
    hub_slot = hub - side * mates
    loads = [
        pltpu.make_async_copy(src, dst, load_sem.at[n])
        for n, (src, dst) in enumerate((
            (right_hbm, right_ref), (left_hbm, left_ref), (x_hbm, x_ref), (group_hbm, group_ref),
            (first_hbm.at[side], first), (gather_hbm.at[side], gather), (near_hbm.at[side], near), (spread_hbm.at[side], spread),
        ))
    ]
    for load in loads:
        load.start()
    others = [lax.rem(me + d, peers) for d in range(1, peers)]
    devices = peers * experts
    here = mine * peers + me
    mate_slots = [lax.rem(hub_slot + d, mates) for d in range(1, mates)]

    def who_index(who):
        return jnp.where(who > hub_slot, who - 1, who)

    def remote(src, dst, send_sem, recv_sem, peer):
        return pltpu.make_async_remote_copy(
            src_ref=src, dst_ref=dst, send_sem=send_sem, recv_sem=recv_sem,
            device_id={"row": peer}, device_id_type=MESH,
        )

    def to_hub(s, k, who):
        piece = cols.at[s, k, who]
        return remote(piece, piece, send1.at[s], recv1.at[s, k, who_index(who)], hub)

    def all_to_hub(s):
        piece = cols.at[s, :, slot]
        return remote(piece, piece, send1.at[s], recv1.at[s, 0, 0], hub)

    def from_hub(s, k, who):
        return remote(
            cols.at[s, k, who], cols.at[s, k, hub_slot], send2.at[s, who_index(who)], recv2.at[s, k // PACK],
            side * mates + who,
        )

    def all_from_hub(s, who):
        piece = cols.at[s, :, who]
        return remote(piece, piece, send2.at[s, who_index(who)], recv2.at[s, 0], side * mates + who)

    def four_from_hub(s, kk):
        piece = cols.at[s, pl.ds(kk * PACK, PACK), hub_slot]
        return remote(piece, piece, send2.at[s, 0], recv2.at[s, kk], hub)

    def across(s, k):
        return remote(out_s.at[s, k], in_s.at[s, k], send_s.at[s], recv_s.at[s, k], far_hub)

    def across_part(s, k, low):
        at = pl.ds(0, alone) if low else pl.ds(alone, gather.shape[0] - alone)
        return remote(
            out_s.at[s, k, at], in_s.at[s, k, at], send_s.at[s],
            recv_first.at[s, k] if low else recv_s.at[s, k], far_hub,
        )

    def all_across(s):
        return remote(out_s.at[s], in_s.at[s], send_s.at[s], recv_s.at[s, 0], far_hub)

    def share_peak(t, s, peer):
        piece = peaks.at[t, s]
        return remote(piece, piece, send3.at[peer], recv3.at[t, s], peer)

    def all_peaks(peer):
        return remote(peaks.at[side], peaks.at[side], send3.at[peer], recv3.at[0, 0], peer)

    def wrap(value, bound):
        return jnp.where(value >= bound, value - bound, value)

    def each_other(act):
        def step(e):
            for r in range(peers):
                place = {"expert": wrap(mine + e, experts), "row": wrap(me + r, peers)}
                if r:
                    act(place)
                else:
                    pl.when(e > 0)(lambda: act(place))

        loop(experts, step)

    def share_sum(place):
        piece = sums.at[here]
        return pltpu.make_async_remote_copy(
            src_ref=piece, dst_ref=piece, send_sem=send4, recv_sem=recv4, device_id=place, device_id_type=MESH
        )

    def all_sums():
        piece = sums.at[pl.ds(0, devices - 1)]
        return pltpu.make_async_remote_copy(
            src_ref=piece, dst_ref=piece, send_sem=send4, recv_sem=recv4, device_id={"row": others[0]},
            device_id_type=MESH,
        )

    barrier = pltpu.get_barrier_semaphore()

    each_other(lambda place: pl.semaphore_signal(barrier, inc=1, device_id=place, device_id_type=MESH))
    loads[0].wait()
    build_column(right_ref, h_ref, 1.0 / math.sqrt(width * HB))
    loads[1].wait()
    build_left(left_ref, left)
    loads[2].wait()

    def column_side(q):
        def step(j):
            low = jnp.dot(x_ref[j, :, :half], h_ref[0, q], preferred_element_type=jnp.float32)
            high = jnp.dot(x_ref[j, :, half:], h_ref[1, q], preferred_element_type=jnp.float32)
            sign = jnp.concatenate([left[j]] * (SLAB // LANES), axis=1)
            for s, both in ((q, low + high), (q + pairs, low - high)):
                both = both * sign
                parts = fold_rows([both[k * SUB:(k + 1) * SUB] for k in range(FOLD)])
                for k in range(FOLD):
                    cols[s, k, slot, pl.ds(pl.multiple_of(j * SUB, SUB), SUB), :] = parts[k].astype(jnp.bfloat16)

        loop(blocks, step)

    def send_slab(s):
        loop(FOLD, lambda k: to_hub(s, k, slot).start())

    def forward(s, k):
        for who in mate_slots:
            to_hub(s, k, who).wait_recv()

        def full():
            z = cols[s, k].reshape(mates * rows, SLAB)
            r = jnp.dot(gather[...], z, preferred_element_type=jnp.float32)
            out_s[s, k] = r.astype(jnp.bfloat16)
            across(s, k).start()

        def remainder():
            z = cols[s, k].reshape(mates * rows, SLAB)
            r = jnp.dot(gather[alone:, :], z, preferred_element_type=jnp.float32)
            out_s[s, k, alone:, :] = r.astype(jnp.bfloat16)
            across_part(s, k, False).start()

        if early:
            pl.when(s < early)(remainder)
            pl.when(s >= early)(full)
        else:
            full()

    def forward_alone(s, k):
        r = jnp.dot(first[...], cols[s, k, hub_slot], preferred_element_type=jnp.float32)
        out_s[s, k, :alone, :] = r.astype(jnp.bfloat16)
        across_part(s, k, True).start()

    def backward(s, k):
        if early:
            @pl.when(s < early)
            def _():
                across_part(s, k, True).wait_recv()
                across_part(s, k, False).wait_recv()

            pl.when(s >= early)(lambda: across(s, k).wait_recv())
        else:
            across(s, k).wait_recv()
        z = cols[s, k].reshape(mates * rows, SLAB)
        r = jnp.dot(near[...], z, preferred_element_type=jnp.float32)
        r = r + jnp.dot(spread[...], in_s[s, k], preferred_element_type=jnp.float32)
        cols[s, k] = r.astype(jnp.bfloat16).reshape(mates, rows, SLAB)
        peak_ref[...] = jnp.maximum(peak_ref[...], jnp.max(jnp.abs(r).reshape(-1, 8, SLAB), axis=0))

        @pl.when(k == FOLD - 1)
        def _():
            peaks[side, s] = jnp.broadcast_to(jnp.max(peak_ref[...], axis=0, keepdims=True), (8, SLAB))
            for peer in others:
                share_peak(side, s, peer).start()

        for who in mate_slots:
            from_hub(s, k, who).start()

    def group_scale(first, count):
        span = count * SLAB
        slab = [jnp.clip(first + i, 0, slabs - 1) for i in range(count)]
        top = jnp.concatenate([jnp.maximum(peaks[0, t], peaks[1, t])[:1] for t in slab], axis=1)
        group = jnp.concatenate(
            [group_ref[:, pl.ds(pl.multiple_of(t * SLAB, SLAB), SLAB)] for t in slab], axis=1
        )
        inside = group == iota((GROUPS, span), 0)
        return jnp.maximum(jnp.max(jnp.where(inside, top, 0.0), axis=1, keepdims=True), 1.0)

    total_rows = peers * blocks * HB
    early = EARLY if alone else 0
    unroll = next(u for u in (7, 1) if blocks % u == 0)

    def scale_slab(s):
        last = jnp.minimum(s + 1, slabs - 1)

        def peak_in(t):
            @pl.when(jnp.logical_or(jnp.logical_not(is_hub), side != t))
            def _():
                @pl.when(s == 0)
                def _():
                    share_peak(t, 0, me).wait_recv()

                @pl.when(s + 1 < slabs)
                def _():
                    share_peak(t, last, me).wait_recv()

        for t in range(2):
            peak_in(t)
        factor = 2.0 / group_scale(s - 1, 3)
        wide = group_ref[:, pl.ds(pl.multiple_of(s * SLAB, SLAB), SLAB)] == iota((GROUPS, SLAB), 0)
        natural_ref[pl.ds(s % 2, 1), :] = jnp.max(jnp.where(wide, factor, 0.0), axis=0, keepdims=True)
        wide = planar_group[pl.ds(s, 1), :] == iota((GROUPS, OCT * LANES), 0).astype(jnp.float32)
        factor_ref[...] = jnp.max(jnp.where(wide, factor, 0.0), axis=0, keepdims=True)

    def permute(s, kk):
        @pl.when(jnp.logical_not(is_hub))
        def _():
            four_from_hub(s, kk).wait_recv()

        both = jnp.concatenate([cols[s, kk * PACK + g, hub_slot] for g in range(PACK)], axis=1)
        planar_ref[s % 2, kk] = jnp.dot(both, p_ref[...], preferred_element_type=jnp.float32)

    def write_scaled(s, kk):
        at_slab = pl.ds(pl.multiple_of(s * SLAB, SLAB), SLAB)
        natural = natural_ref[pl.ds(s % 2, 1), :]

        def tile(j):
            at = pl.ds(pl.multiple_of(j * SUB, SUB), SUB)
            for g in range(PACK):
                value = cols[s, kk * PACK + g, hub_slot, at, :].astype(jnp.float32) * natural
                scaled_ref[j, kk * PACK + g, :, at_slab] = value.astype(jnp.bfloat16)

        def some(i):
            for u in range(unroll):
                tile(i * unroll + u)

        loop(blocks // unroll, some)

    def lattice(s, kk):
        octets = SLAB // OCT
        lane = iota((SUB, LANES), 1)
        place = s % PACK
        inside = lane // octets == place
        at_error = pl.ds(pl.multiple_of(s // PACK * LANES, LANES), LANES)
        row = (me * (blocks * HB) + (kk * PACK + lane // octets) * SUB + iota((SUB, LANES), 0)).astype(jnp.float32)
        weight = (1.0 + 4.0 * (row + 0.5) / total_rows) / 3.0

        def tile(j):
            at = pl.ds(pl.multiple_of(j * SUB, SUB), SUB)
            square = near_sum = low = size = most = least = None
            for c in range(OCT):
                value = planar_ref[s % 2, kk, at, c * LANES:(c + 1) * LANES] * factor_ref[:, c * LANES:(c + 1) * LANES]
                nearest = jnp.round(value)
                offset = jnp.abs(value - nearest)
                below = jnp.floor(value)
                if c == 0:
                    square, near_sum, low, size = offset * offset, nearest, below, offset
                    most = least = offset
                else:
                    square, near_sum, low = square + offset * offset, near_sum + nearest, low + below
                    size = size + offset
                    most, least = jnp.maximum(most, offset), jnp.minimum(least, offset)
            odd = near_sum - 2.0 * jnp.floor(near_sum * 0.5) > 0.5
            whole = jnp.where(odd, square + (1.0 - 2.0 * most), square)
            shifted = square + (OCT * 0.25 - size)
            odd = low - 2.0 * jnp.floor(low * 0.5) > 0.5
            error = jnp.minimum(whole, jnp.where(odd, shifted + 2.0 * least, shifted))
            for g in range(PACK):
                turned = pltpu.roll(error, lax.rem(place + PACK - g, PACK) * octets, 1)
                old = error_ref[j, kk * PACK + g, :, at_error]
                error_ref[j, kk * PACK + g, :, at_error] = jnp.where(inside, turned, old)
            return error * (weight + j.astype(jnp.float32) * (4.0 * HB / (3.0 * total_rows)))

        def some(i):
            parts = [tile(i * unroll + u) for u in range(unroll)]
            sum_ref[...] += sum(parts[1:], parts[0])

        loop(blocks // unroll, some)

    column_side(0)
    pl.semaphore_wait(barrier, devices - 1)

    @pl.when(jnp.logical_not(is_hub))
    def _():
        send_slab(0)

        def step(q):
            column_side(q + 1)
            send_slab(q + 1)

        loop(pairs - 1, step)
        loop(slabs - pairs, lambda q: send_slab(q + pairs))

    for load in loads[3:]:
        load.wait()

    @pl.when(is_hub)
    def _():
        def begin(s):
            pl.when(s > 0)(lambda: column_side(s))
            if early:
                loop(FOLD, lambda k: forward_alone(s, k))

        loop(EARLY, begin)
        loop(LEAD, lambda k: forward(0, k))

    build_order(p_ref)
    sum_ref[...] = jnp.zeros_like(sum_ref)
    row = jnp.concatenate([group_ref[:, s * SLAB:(s + 1) * SLAB] for s in range(slabs)], axis=0)
    row = jnp.concatenate([row.astype(jnp.float32).astype(jnp.bfloat16)] * PACK, axis=1)
    planar_group[...] = jnp.dot(row, p_ref[...], preferred_element_type=jnp.float32)

    def stage(t):
        mixes = jnp.logical_and(is_hub, t < slabs)

        @pl.when(mixes)
        def _():
            peak_ref[...] = jnp.zeros_like(peak_ref)

        @pl.when(jnp.logical_and(is_hub, jnp.logical_and(t + 1 >= EARLY, t + 1 < pairs)))
        def _():
            column_side(t + 1)

        def part(kk):
            @pl.when(mixes)
            def _():
                def step(i):
                    k = kk * PACK + i
                    ahead = t * FOLD + k + LEAD

                    @pl.when(ahead < slabs * FOLD)
                    def _():
                        forward(ahead // FOLD, ahead % FOLD)

                    backward(t, k)

                loop(PACK, step)

            @pl.when(t >= 2)
            def _():
                @pl.when(kk == 0)
                def _():
                    scale_slab(t - 2)

                lattice(t - 2, kk)
                pl.when(t < slabs)(lambda: write_scaled(t - 2, kk))

            come = jnp.where(is_hub, t, t - kk)

            @pl.when(jnp.logical_and(come >= 0, come < slabs))
            def _():
                permute(come, kk)

        loop(FOLD // PACK, part)

    loop(slabs + 2, stage)


    part = jnp.sum(jnp.sum(sum_ref[...], axis=0, keepdims=True), axis=1, keepdims=True)
    sums[here] = jnp.broadcast_to(part / (total_rows * width // OCT), (1, LANES))
    each_other(lambda place: share_sum(place).start())
    loop(FOLD // PACK, lambda kk: write_scaled(slabs - 2, kk))
    loop(FOLD // PACK, lambda kk: write_scaled(slabs - 1, kk))
    peak = group_scale(0, slabs) * 0.5
    scale_ref[...] = jnp.broadcast_to(peak, (GROUPS, LANES)).T[:1, :GROUPS]

    @pl.when(jnp.logical_not(is_hub))
    def _():
        loop(slabs, lambda s: all_to_hub(s).wait_send())

    @pl.when(is_hub)
    def _():
        for peer in others:
            all_peaks(peer).wait_send()

        def drain(s):
            all_across(s).wait_send()
            for who in mate_slots:
                all_from_hub(s, who).wait_send()

        loop(slabs, drain)

    all_sums().wait_recv()
    total = jnp.sum(sums[...], axis=0)
    mean = jnp.sum(sums[pl.ds(mine * peers, peers)], axis=0)
    mean_ref[0] = jnp.max(mean)
    total_ref[0] = jnp.max(total / experts)

    all_sums().wait_send()


def put_kernel(scaled_ref, error_ref, scale_ref, scaled_out, error_out, scale_out, sems):
    pairs = ((scale_ref, scale_out), (scaled_ref, scaled_out), (error_ref, error_out))
    copies = [pltpu.make_async_copy(src, dst, sems.at[n]) for n, (src, dst) in enumerate(pairs)]
    for copy in copies:
        copy.start()
    for copy in copies:
        copy.wait()


def put(*results):
    count = len(results)
    return pl.pallas_call(
        put_kernel,
        out_shape=tuple(jax.ShapeDtypeStruct(r.shape, r.dtype) for r in results),
        in_specs=[pl.BlockSpec(memory_space=pltpu.VMEM)] * count,
        out_specs=[pl.BlockSpec(memory_space=pl.ANY)] * count,
        scratch_shapes=[pltpu.SemaphoreType.DMA((count,))],
        compiler_params=pltpu.CompilerParams(vmem_limit_bytes=16 * 2**20),
    )(*results)


def body(weights, left_bits, right_bits, groups):
    _, local_rows, width = weights.shape
    peers = lax.axis_size("row")
    experts = lax.axis_size("expert")
    blocks = local_rows // HB
    half = width // 2
    mates = peers // 2
    rows = blocks * SUB
    slabs = width // SLAB
    (near, gather, spread), first = row_tables(BLOCKS, blocks)
    alone = first.shape[1]
    first = first if alone else gather
    inner, reach = mates * rows, gather.shape[1]
    vmem = pl.BlockSpec(memory_space=pltpu.VMEM)
    hbm = pl.BlockSpec(memory_space=pl.ANY)
    dma = pltpu.SemaphoreType.DMA
    smem = pl.BlockSpec(memory_space=pltpu.SMEM)
    scaled, errors, group_scale, mean, total = pl.pallas_call(
        functools.partial(kernel, peers, experts, alone),
        out_shape=(
            pltpu.VMEM((blocks, FOLD, SUB, width), jnp.bfloat16),
            pltpu.VMEM((blocks, FOLD, SUB, width // OCT), jnp.float32),
            pltpu.VMEM((1, GROUPS), jnp.float32),
            jax.ShapeDtypeStruct((1,), jnp.float32),
            jax.ShapeDtypeStruct((1,), jnp.float32),
        ),
        in_specs=[hbm] * 8,
        out_specs=(vmem, vmem, vmem, smem, smem),
        scratch_shapes=[
            pltpu.VMEM((blocks, HB, width), jnp.bfloat16),
            pltpu.VMEM((1, local_rows), jnp.int32),
            pltpu.VMEM((1, width), jnp.int32),
            pltpu.VMEM((1, width), jnp.int32),
            pltpu.VMEM((inner, inner), jnp.bfloat16),
            pltpu.VMEM((reach, inner), jnp.bfloat16),
            pltpu.VMEM((inner, reach), jnp.bfloat16),
            pltpu.VMEM(first.shape[1:], jnp.bfloat16),
            pltpu.VMEM((blocks, HB, LANES), jnp.float32),
            pltpu.VMEM((2, slabs // 2, half, SLAB), jnp.bfloat16),
            pltpu.VMEM((PACK * SLAB, OCT * LANES), jnp.bfloat16),
            pltpu.VMEM((slabs, FOLD, mates, rows, SLAB), jnp.bfloat16),
            pltpu.VMEM((slabs, FOLD, reach, SLAB), jnp.bfloat16),
            pltpu.VMEM((slabs, FOLD, reach, SLAB), jnp.bfloat16),
            pltpu.VMEM((2, FOLD // PACK, rows, OCT * LANES), jnp.float32),
            pltpu.VMEM((slabs, OCT * LANES), jnp.float32),
            pltpu.VMEM((2, slabs, 8, SLAB), jnp.float32),
            pltpu.VMEM((8, SLAB), jnp.float32),
            pltpu.VMEM((2, SLAB), jnp.float32),
            pltpu.VMEM((1, OCT * LANES), jnp.float32),
            pltpu.VMEM((SUB, LANES), jnp.float32),
            pltpu.VMEM((peers * experts, 1, LANES), jnp.float32),
            dma((slabs,)),
            dma((slabs, FOLD, max(mates - 1, 1))),
            dma((slabs, max(mates - 1, 1))),
            dma((slabs, FOLD // PACK)),
            dma((peers,)),
            dma((2, slabs)),
            dma((slabs,)),
            dma((slabs, FOLD)),
            dma((EARLY, FOLD)),
            dma,
            dma,
            dma((8,)),
        ],
        compiler_params=pltpu.CompilerParams(
            collective_id=0, has_side_effects=True, vmem_limit_bytes=54 * 2**20
        ),
    )(weights.reshape(blocks, HB, width), left_bits, right_bits, groups, near, gather, spread, first)
    scaled, errors, group_scale = put(scaled, errors, group_scale)
    return (
        scaled.reshape(1, local_rows, width),
        errors.reshape(1, local_rows, width // OCT),
        group_scale,
        mean,
        total.reshape(()),
    )


def solution(mesh):
    placed = (P("expert", "row", None), P("expert", "row"), P("expert", None), P("expert", None))
    return jax.shard_map(
        body,
        mesh=mesh,
        in_specs=placed,
        out_specs=(
            P("expert", "row", None),
            P("expert", "row", None),
            P("expert", None),
            P("expert"),
            P(),
        ),
        check_vma=False,
    )
```

```python
import functools
import math

import jax
import jax.numpy as jnp
import numpy as np
from jax import lax
from jax.experimental import pallas as pl
from jax.experimental.pallas import tpu as pltpu
from jax.sharding import PartitionSpec as P

HB = 128
SUB = 16
FOLD = HB // SUB
OCT = 8
LANES = 128
GROUPS = 16
BLOCKS = 56
SLAB = 256
PACK = LANES * OCT // SLAB
LEAD = 3
EARLY = 2
MESH = pl.DeviceIdType.MESH


def signs(common, bits):
    for shift in (4, 2, 1):
        if shift < bits:
            common = common ^ (common >> shift)
    return (1 - 2 * (common & 1)).astype(jnp.float32)


def iota(shape, dim):
    return lax.broadcasted_iota(jnp.int32, shape, dim)


def down(row):
    return jnp.broadcast_to(row, (LANES, LANES)).T


def cosine_table(order):
    first = np.arange(order, dtype=np.float64)[:, None]
    second = np.arange(order, dtype=np.float64)[None, :]
    table = math.sqrt(2.0 / order) * np.cos(math.pi * (2.0 * second + 1.0) * first / (2.0 * order))
    return np.where(first == 0.0, table * math.sqrt(0.5), table)


def cross_factors(order, to, own):
    half = order // 2
    block = cosine_table(order)[to * half:(to + 1) * half, (1 - to) * half:(2 - to) * half]
    even, odd = block[0::2], block[1::2]
    along = odd @ even.T / np.sum(even * even, axis=1)
    _, s, v = np.linalg.svd(odd - along @ even)
    kept = int(np.sum(s > 2.0 ** -24))
    basis = np.concatenate([even / np.sqrt(np.sum(even * even, axis=1, keepdims=True)), v[:kept]])
    far = slice(0, half - own) if to else slice(own, half)
    alone = max(0, basis.shape[0] - (half - own))
    if alone:
        turn = np.linalg.svd(basis[:, far].T)[2][::-1]
        basis = turn @ basis
        basis[:alone, far] = 0.0
    return basis, block @ basis.T, alone


def row_tables(order, own):
    half = order // 2
    table = cosine_table(order)
    near = np.stack([table[s * half:(s + 1) * half, s * half:(s + 1) * half] for s in range(2)])
    to_low, to_high = cross_factors(order, 0, own), cross_factors(order, 1, own)
    gather = np.stack([to_high[0], to_low[0]])
    spread = np.stack([to_low[1], to_high[1]])
    index = np.arange(SUB)
    inner = np.array([[1 - 2 * (bin(a & b).count("1") & 1) for b in index] for a in index], np.float32)
    tables = [
        np.stack([np.kron(t, m) for t in ts]).astype(np.float32).astype(np.dtype(jnp.bfloat16))
        for ts, m in ((near, inner), (gather, inner), (spread, np.eye(SUB, dtype=np.float32)))
    ]
    alone = to_high[2] * SUB
    first = np.stack([tables[1][0][:alone, (half - own) * SUB:], tables[1][1][:alone, :own * SUB]])
    return tables, first


def build_column(right_ref, h_ref, scale):
    half = h_ref.shape[2]
    square = (LANES, LANES)
    inner = signs(iota(square, 0) & iota(square, 1), 7)

    def step(u, _):
        at = pl.ds(pl.multiple_of(u * LANES, LANES), LANES)
        for side in range(2):
            bits = right_ref[:, pl.ds(pl.multiple_of(side * half + u * LANES, LANES), LANES)]
            part = inner * down((2 * bits - 1).astype(jnp.float32) * scale)
            for v in range(half // LANES):
                common = u & v
                common = common ^ (common >> 4)
                common = common ^ (common >> 2)
                common = common ^ (common >> 1)
                sign = (1 - 2 * (common & 1)).astype(jnp.float32)
                q, c = v * LANES // SLAB, v * LANES % SLAB
                h_ref[side, q, at, c:c + LANES] = (part * sign).astype(jnp.bfloat16)
        return 0

    lax.fori_loop(0, half // LANES, step, 0)


def build_left(left_ref, left):
    def step(j, _):
        bits = left_ref[:, pl.ds(pl.multiple_of(j * HB, HB), HB)]
        left[j] = down((2 * bits - 1).astype(jnp.float32))
        return 0

    lax.fori_loop(0, left.shape[0], step, 0)


def build_order(p_ref):
    size = p_ref.shape[0]
    octets = SLAB // OCT

    def step(s, _):
        lane = iota((size, LANES), 1)
        wanted = lane // octets * SLAB + lane % octets * OCT + s
        hit = (wanted == iota((size, LANES), 0)).astype(jnp.float32)
        p_ref[:, pl.ds(pl.multiple_of(s * LANES, LANES), LANES)] = hit.astype(jnp.bfloat16)
        return 0

    lax.fori_loop(0, OCT, step, 0)


def fold_rows(parts):
    step = 1
    while step < len(parts):
        mixed = list(parts)
        for k in range(len(parts)):
            if not k & step:
                mixed[k] = parts[k] + parts[k + step]
                mixed[k + step] = parts[k] - parts[k + step]
        parts, step = mixed, 2 * step
    return parts


def loop(count, step):
    def run(i, _):
        step(i)
        return 0

    lax.fori_loop(0, count, run, 0)


def kernel(
    peers, experts, alone, x_hbm, left_hbm, right_hbm, group_hbm, near_hbm, gather_hbm, spread_hbm, first_hbm,
    scaled_ref, error_ref, scale_ref, mean_ref, total_ref,
    x_ref, left_ref, right_ref, group_ref, near, gather, spread, first,
    left, h_ref, p_ref, cols, out_s, in_s, planar_ref, planar_group, peaks, peak_ref, natural_ref, factor_ref,
    sum_ref, sums,
    send1, recv1, send2, recv2, send3, recv3, send_s, recv_s, recv_first, send4, recv4, load_sem,
):
    blocks, _, width = x_ref.shape
    half = width // 2
    slabs = width // SLAB
    pairs = slabs // 2
    mates = peers // 2
    rows = blocks * SUB
    me = lax.axis_index("row")
    mine = lax.axis_index("expert")
    side = me // mates
    slot = me - side * mates
    hub = mates - 1 + side
    far_hub = mates - side
    is_hub = me == hub
    hub_slot = hub - side * mates
    loads = [
        pltpu.make_async_copy(src, dst, load_sem.at[n])
        for n, (src, dst) in enumerate((
            (right_hbm, right_ref), (left_hbm, left_ref), (x_hbm, x_ref), (group_hbm, group_ref),
            (first_hbm.at[side], first), (gather_hbm.at[side], gather), (near_hbm.at[side], near), (spread_hbm.at[side], spread),
        ))
    ]
    for load in loads:
        load.start()
    others = [lax.rem(me + d, peers) for d in range(1, peers)]
    devices = peers * experts
    here = mine * peers + me
    mate_slots = [lax.rem(hub_slot + d, mates) for d in range(1, mates)]

    def who_index(who):
        return jnp.where(who > hub_slot, who - 1, who)

    def remote(src, dst, send_sem, recv_sem, peer):
        return pltpu.make_async_remote_copy(
            src_ref=src, dst_ref=dst, send_sem=send_sem, recv_sem=recv_sem,
            device_id={"row": peer}, device_id_type=MESH,
        )

    def to_hub(s, k, who):
        piece = cols.at[s, k, who]
        return remote(piece, piece, send1.at[s], recv1.at[s, k, who_index(who)], hub)

    def all_to_hub(s):
        piece = cols.at[s, :, slot]
        return remote(piece, piece, send1.at[s], recv1.at[s, 0, 0], hub)

    def from_hub(s, k, who):
        return remote(
            cols.at[s, k, who], cols.at[s, k, hub_slot], send2.at[s, who_index(who)], recv2.at[s, k // PACK],
            side * mates + who,
        )

    def all_from_hub(s, who):
        piece = cols.at[s, :, who]
        return remote(piece, piece, send2.at[s, who_index(who)], recv2.at[s, 0], side * mates + who)

    def four_from_hub(s, kk):
        piece = cols.at[s, pl.ds(kk * PACK, PACK), hub_slot]
        return remote(piece, piece, send2.at[s, 0], recv2.at[s, kk], hub)

    def across(s, k):
        return remote(out_s.at[s, k], in_s.at[s, k], send_s.at[s], recv_s.at[s, k], far_hub)

    def across_part(s, k, low):
        at = pl.ds(0, alone) if low else pl.ds(alone, gather.shape[0] - alone)
        return remote(
            out_s.at[s, k, at], in_s.at[s, k, at], send_s.at[s],
            recv_first.at[s, k] if low else recv_s.at[s, k], far_hub,
        )

    def all_across(s):
        return remote(out_s.at[s], in_s.at[s], send_s.at[s], recv_s.at[s, 0], far_hub)

    def share_peak(t, s, peer):
        piece = peaks.at[t, s]
        return remote(piece, piece, send3.at[peer], recv3.at[t, s], peer)

    def all_peaks(peer):
        return remote(peaks.at[side], peaks.at[side], send3.at[peer], recv3.at[0, 0], peer)

    def wrap(value, bound):
        return jnp.where(value >= bound, value - bound, value)

    def each_other(act):
        def step(e):
            for r in range(peers):
                place = {"expert": wrap(mine + e, experts), "row": wrap(me + r, peers)}
                if r:
                    act(place)
                else:
                    pl.when(e > 0)(lambda: act(place))

        loop(experts, step)

    def share_sum(place):
        piece = sums.at[here]
        return pltpu.make_async_remote_copy(
            src_ref=piece, dst_ref=piece, send_sem=send4, recv_sem=recv4, device_id=place, device_id_type=MESH
        )

    def all_sums():
        piece = sums.at[pl.ds(0, devices - 1)]
        return pltpu.make_async_remote_copy(
            src_ref=piece, dst_ref=piece, send_sem=send4, recv_sem=recv4, device_id={"row": others[0]},
            device_id_type=MESH,
        )

    barrier = pltpu.get_barrier_semaphore()

    each_other(lambda place: pl.semaphore_signal(barrier, inc=1, device_id=place, device_id_type=MESH))
    loads[0].wait()
    build_column(right_ref, h_ref, 1.0 / math.sqrt(width * HB))
    loads[1].wait()
    build_left(left_ref, left)
    loads[2].wait()

    def column_side(q):
        def step(j):
            low = jnp.dot(x_ref[j, :, :half], h_ref[0, q], preferred_element_type=jnp.float32)
            high = jnp.dot(x_ref[j, :, half:], h_ref[1, q], preferred_element_type=jnp.float32)
            sign = jnp.concatenate([left[j]] * (SLAB // LANES), axis=1)
            for s, both in ((q, low + high), (q + pairs, low - high)):
                both = both * sign
                parts = fold_rows([both[k * SUB:(k + 1) * SUB] for k in range(FOLD)])
                for k in range(FOLD):
                    cols[s, k, slot, pl.ds(pl.multiple_of(j * SUB, SUB), SUB), :] = parts[k].astype(jnp.bfloat16)

        loop(blocks, step)

    def send_slab(s):
        loop(FOLD, lambda k: to_hub(s, k, slot).start())

    def forward(s, k):
        for who in mate_slots:
            to_hub(s, k, who).wait_recv()

        def full():
            z = cols[s, k].reshape(mates * rows, SLAB)
            r = jnp.dot(gather[...], z, preferred_element_type=jnp.float32)
            out_s[s, k] = r.astype(jnp.bfloat16)
            across(s, k).start()

        def remainder():
            z = cols[s, k].reshape(mates * rows, SLAB)
            r = jnp.dot(gather[alone:, :], z, preferred_element_type=jnp.float32)
            out_s[s, k, alone:, :] = r.astype(jnp.bfloat16)
            across_part(s, k, False).start()

        if early:
            pl.when(s < early)(remainder)
            pl.when(s >= early)(full)
        else:
            full()

    def forward_alone(s, k):
        r = jnp.dot(first[...], cols[s, k, hub_slot], preferred_element_type=jnp.float32)
        out_s[s, k, :alone, :] = r.astype(jnp.bfloat16)
        across_part(s, k, True).start()

    def backward(s, k):
        if early:
            @pl.when(s < early)
            def _():
                across_part(s, k, True).wait_recv()
                across_part(s, k, False).wait_recv()

            pl.when(s >= early)(lambda: across(s, k).wait_recv())
        else:
            across(s, k).wait_recv()
        z = cols[s, k].reshape(mates * rows, SLAB)
        r = jnp.dot(near[...], z, preferred_element_type=jnp.float32)
        r = r + jnp.dot(spread[...], in_s[s, k], preferred_element_type=jnp.float32)
        cols[s, k] = r.astype(jnp.bfloat16).reshape(mates, rows, SLAB)
        peak_ref[...] = jnp.maximum(peak_ref[...], jnp.max(jnp.abs(r).reshape(-1, 8, SLAB), axis=0))

        @pl.when(k == FOLD - 1)
        def _():
            peaks[side, s] = jnp.broadcast_to(jnp.max(peak_ref[...], axis=0, keepdims=True), (8, SLAB))
            for peer in others:
                share_peak(side, s, peer).start()

        for who in mate_slots:
            from_hub(s, k, who).start()

    def group_scale(first, count):
        span = count * SLAB
        slab = [jnp.clip(first + i, 0, slabs - 1) for i in range(count)]
        top = jnp.concatenate([jnp.maximum(peaks[0, t], peaks[1, t])[:1] for t in slab], axis=1)
        group = jnp.concatenate(
            [group_ref[:, pl.ds(pl.multiple_of(t * SLAB, SLAB), SLAB)] for t in slab], axis=1
        )
        inside = group == iota((GROUPS, span), 0)
        return jnp.maximum(jnp.max(jnp.where(inside, top, 0.0), axis=1, keepdims=True), 1.0)

    total_rows = peers * blocks * HB
    early = EARLY if alone else 0
    unroll = next(u for u in (14, 7, 1) if blocks % u == 0)

    def peaks_in(s):
        last = jnp.minimum(s + 1, slabs - 1)

        def peak_in(t):
            @pl.when(jnp.logical_or(jnp.logical_not(is_hub), side != t))
            def _():
                @pl.when(s == 0)
                def _():
                    share_peak(t, 0, me).wait_recv()

                @pl.when(s + 1 < slabs)
                def _():
                    share_peak(t, last, me).wait_recv()

        for t in range(2):
            peak_in(t)

    def scale_slab(s):
        factor = 2.0 / group_scale(s - 1, 3)
        wide = group_ref[:, pl.ds(pl.multiple_of(s * SLAB, SLAB), SLAB)] == iota((GROUPS, SLAB), 0)
        natural_ref[pl.ds(s % 2, 1), :] = jnp.max(jnp.where(wide, factor, 0.0), axis=0, keepdims=True)
        wide = planar_group[pl.ds(s, 1), :] == iota((GROUPS, OCT * LANES), 0).astype(jnp.float32)
        factor_ref[s % 2] = jnp.max(jnp.where(wide, factor, 0.0), axis=0, keepdims=True)

    def permute(s, kk):
        @pl.when(jnp.logical_not(is_hub))
        def _():
            four_from_hub(s, kk).wait_recv()

        both = jnp.concatenate([cols[s, kk * PACK + g, hub_slot] for g in range(PACK)], axis=1)
        planar_ref[s % 2, kk] = jnp.dot(both, p_ref[...], preferred_element_type=jnp.float32)

    def write_scaled(s, kk):
        at_slab = pl.ds(pl.multiple_of(s * SLAB, SLAB), SLAB)
        natural = natural_ref[pl.ds(s % 2, 1), :]

        def tile(j):
            at = pl.ds(pl.multiple_of(j * SUB, SUB), SUB)
            for g in range(PACK):
                value = cols[s, kk * PACK + g, hub_slot, at, :].astype(jnp.float32) * natural
                scaled_ref[j, kk * PACK + g, :, at_slab] = value.astype(jnp.bfloat16)

        def some(i):
            for u in range(unroll):
                tile(i * unroll + u)

        loop(blocks // unroll, some)

    def lattice(s, kk):
        octets = SLAB // OCT
        lane = iota((SUB, LANES), 1)
        place = s % PACK
        inside = lane // octets == place
        at_error = pl.ds(pl.multiple_of(s // PACK * LANES, LANES), LANES)
        row = (me * (blocks * HB) + (kk * PACK + lane // octets) * SUB + iota((SUB, LANES), 0)).astype(jnp.float32)
        weight = (1.0 + 4.0 * (row + 0.5) / total_rows) / 3.0

        def tile(j):
            at = pl.ds(pl.multiple_of(j * SUB, SUB), SUB)
            square = near_sum = low = size = most = least = None
            for c in range(OCT):
                value = planar_ref[s % 2, kk, at, c * LANES:(c + 1) * LANES] * factor_ref[s % 2, :, c * LANES:(c + 1) * LANES]
                nearest = jnp.round(value)
                offset = jnp.abs(value - nearest)
                below = jnp.floor(value)
                if c == 0:
                    square, near_sum, low, size = offset * offset, nearest, below, offset
                    most = least = offset
                else:
                    square, near_sum, low = square + offset * offset, near_sum + nearest, low + below
                    size = size + offset
                    most, least = jnp.maximum(most, offset), jnp.minimum(least, offset)
            odd = near_sum - 2.0 * jnp.floor(near_sum * 0.5) > 0.5
            whole = jnp.where(odd, square + (1.0 - 2.0 * most), square)
            shifted = square + (OCT * 0.25 - size)
            odd = low - 2.0 * jnp.floor(low * 0.5) > 0.5
            error = jnp.minimum(whole, jnp.where(odd, shifted + 2.0 * least, shifted))
            for g in range(PACK):
                turned = pltpu.roll(error, lax.rem(place + PACK - g, PACK) * octets, 1)
                old = error_ref[j, kk * PACK + g, :, at_error]
                error_ref[j, kk * PACK + g, :, at_error] = jnp.where(inside, turned, old)
            return error * (weight + j.astype(jnp.float32) * (4.0 * HB / (3.0 * total_rows)))

        def some(i):
            parts = [tile(i * unroll + u) for u in range(unroll)]
            sum_ref[...] += sum(parts[1:], parts[0])

        loop(blocks // unroll, some)

    column_side(0)
    pl.semaphore_wait(barrier, devices - 1)

    @pl.when(jnp.logical_not(is_hub))
    def _():
        send_slab(0)

        def step(q):
            column_side(q + 1)
            send_slab(q + 1)

        loop(pairs - 1, step)
        loop(slabs - pairs, lambda q: send_slab(q + pairs))

    for load in loads[3:]:
        load.wait()

    @pl.when(is_hub)
    def _():
        def begin(s):
            pl.when(s > 0)(lambda: column_side(s))
            if early:
                loop(FOLD, lambda k: forward_alone(s, k))

        loop(EARLY, begin)
        loop(LEAD, lambda k: forward(0, k))

    build_order(p_ref)
    sum_ref[...] = jnp.zeros_like(sum_ref)
    row = jnp.concatenate([group_ref[:, s * SLAB:(s + 1) * SLAB] for s in range(slabs)], axis=0)
    row = jnp.concatenate([row.astype(jnp.float32).astype(jnp.bfloat16)] * PACK, axis=1)
    planar_group[...] = jnp.dot(row, p_ref[...], preferred_element_type=jnp.float32)

    def stage(t):
        mixes = jnp.logical_and(is_hub, t < slabs)

        @pl.when(mixes)
        def _():
            peak_ref[...] = jnp.zeros_like(peak_ref)

        @pl.when(jnp.logical_and(is_hub, jnp.logical_and(t + 1 >= EARLY, t + 1 < pairs)))
        def _():
            column_side(t + 1)

        def part(kk):
            @pl.when(mixes)
            def _():
                def step(i):
                    k = kk * PACK + i
                    ahead = t * FOLD + k + LEAD

                    @pl.when(ahead < slabs * FOLD)
                    def _():
                        forward(ahead // FOLD, ahead % FOLD)

                    backward(t, k)

                loop(PACK, step)

            @pl.when(t >= 2)
            def _():
                @pl.when(jnp.logical_and(kk == 0, t < slabs))
                def _():
                    peaks_in(t - 2)
                    scale_slab(t - 2)

                @pl.when(jnp.logical_and(kk == 0, t == slabs))
                def _():
                    peaks_in(slabs - 2)
                    scale_slab(slabs - 2)
                    scale_slab(slabs - 1)

                lattice(t - 2, kk)
                pl.when(t < slabs)(lambda: write_scaled(t - 2, kk))

            come = jnp.where(is_hub, t, t - kk)

            @pl.when(jnp.logical_and(come >= 0, come < slabs))
            def _():
                permute(come, kk)

        loop(FOLD // PACK, part)

    loop(slabs + 2, stage)


    part = jnp.sum(jnp.sum(sum_ref[...], axis=0, keepdims=True), axis=1, keepdims=True)
    sums[here] = jnp.broadcast_to(part / (total_rows * width // OCT), (1, LANES))
    each_other(lambda place: share_sum(place).start())
    loop(FOLD // PACK, lambda kk: write_scaled(slabs - 2, kk))
    loop(FOLD // PACK, lambda kk: write_scaled(slabs - 1, kk))
    peak = group_scale(0, slabs) * 0.5
    scale_ref[...] = jnp.broadcast_to(peak, (GROUPS, LANES)).T[:1, :GROUPS]

    @pl.when(jnp.logical_not(is_hub))
    def _():
        loop(slabs, lambda s: all_to_hub(s).wait_send())

    @pl.when(is_hub)
    def _():
        for peer in others:
            all_peaks(peer).wait_send()

        def drain(s):
            all_across(s).wait_send()
            for who in mate_slots:
                all_from_hub(s, who).wait_send()

        loop(slabs, drain)

    all_sums().wait_recv()
    total = jnp.sum(sums[...], axis=0)
    mean = jnp.sum(sums[pl.ds(mine * peers, peers)], axis=0)
    mean_ref[0] = jnp.max(mean)
    total_ref[0] = jnp.max(total / experts)

    all_sums().wait_send()


def put_kernel(scaled_ref, error_ref, scale_ref, scaled_out, error_out, scale_out, sems):
    pairs = ((scale_ref, scale_out), (scaled_ref, scaled_out), (error_ref, error_out))
    copies = [pltpu.make_async_copy(src, dst, sems.at[n]) for n, (src, dst) in enumerate(pairs)]
    for copy in copies:
        copy.start()
    for copy in copies:
        copy.wait()


def put(*results):
    count = len(results)
    return pl.pallas_call(
        put_kernel,
        out_shape=tuple(jax.ShapeDtypeStruct(r.shape, r.dtype) for r in results),
        in_specs=[pl.BlockSpec(memory_space=pltpu.VMEM)] * count,
        out_specs=[pl.BlockSpec(memory_space=pl.ANY)] * count,
        scratch_shapes=[pltpu.SemaphoreType.DMA((count,))],
        compiler_params=pltpu.CompilerParams(vmem_limit_bytes=16 * 2**20),
    )(*results)


def body(weights, left_bits, right_bits, groups):
    _, local_rows, width = weights.shape
    peers = lax.axis_size("row")
    experts = lax.axis_size("expert")
    blocks = local_rows // HB
    half = width // 2
    mates = peers // 2
    rows = blocks * SUB
    slabs = width // SLAB
    (near, gather, spread), first = row_tables(BLOCKS, blocks)
    alone = first.shape[1]
    first = first if alone else gather
    inner, reach = mates * rows, gather.shape[1]
    vmem = pl.BlockSpec(memory_space=pltpu.VMEM)
    hbm = pl.BlockSpec(memory_space=pl.ANY)
    dma = pltpu.SemaphoreType.DMA
    smem = pl.BlockSpec(memory_space=pltpu.SMEM)
    scaled, errors, group_scale, mean, total = pl.pallas_call(
        functools.partial(kernel, peers, experts, alone),
        out_shape=(
            pltpu.VMEM((blocks, FOLD, SUB, width), jnp.bfloat16),
            pltpu.VMEM((blocks, FOLD, SUB, width // OCT), jnp.float32),
            pltpu.VMEM((1, GROUPS), jnp.float32),
            jax.ShapeDtypeStruct((1,), jnp.float32),
            jax.ShapeDtypeStruct((1,), jnp.float32),
        ),
        in_specs=[hbm] * 8,
        out_specs=(vmem, vmem, vmem, smem, smem),
        scratch_shapes=[
            pltpu.VMEM((blocks, HB, width), jnp.bfloat16),
            pltpu.VMEM((1, local_rows), jnp.int32),
            pltpu.VMEM((1, width), jnp.int32),
            pltpu.VMEM((1, width), jnp.int32),
            pltpu.VMEM((inner, inner), jnp.bfloat16),
            pltpu.VMEM((reach, inner), jnp.bfloat16),
            pltpu.VMEM((inner, reach), jnp.bfloat16),
            pltpu.VMEM(first.shape[1:], jnp.bfloat16),
            pltpu.VMEM((blocks, HB, LANES), jnp.float32),
            pltpu.VMEM((2, slabs // 2, half, SLAB), jnp.bfloat16),
            pltpu.VMEM((PACK * SLAB, OCT * LANES), jnp.bfloat16),
            pltpu.VMEM((slabs, FOLD, mates, rows, SLAB), jnp.bfloat16),
            pltpu.VMEM((slabs, FOLD, reach, SLAB), jnp.bfloat16),
            pltpu.VMEM((slabs, FOLD, reach, SLAB), jnp.bfloat16),
            pltpu.VMEM((2, FOLD // PACK, rows, OCT * LANES), jnp.float32),
            pltpu.VMEM((slabs, OCT * LANES), jnp.float32),
            pltpu.VMEM((2, slabs, 8, SLAB), jnp.float32),
            pltpu.VMEM((8, SLAB), jnp.float32),
            pltpu.VMEM((2, SLAB), jnp.float32),
            pltpu.VMEM((2, 1, OCT * LANES), jnp.float32),
            pltpu.VMEM((SUB, LANES), jnp.float32),
            pltpu.VMEM((peers * experts, 1, LANES), jnp.float32),
            dma((slabs,)),
            dma((slabs, FOLD, max(mates - 1, 1))),
            dma((slabs, max(mates - 1, 1))),
            dma((slabs, FOLD // PACK)),
            dma((peers,)),
            dma((2, slabs)),
            dma((slabs,)),
            dma((slabs, FOLD)),
            dma((EARLY, FOLD)),
            dma,
            dma,
            dma((8,)),
        ],
        compiler_params=pltpu.CompilerParams(
            collective_id=0, has_side_effects=True, vmem_limit_bytes=54 * 2**20
        ),
    )(weights.reshape(blocks, HB, width), left_bits, right_bits, groups, near, gather, spread, first)
    scaled, errors, group_scale = put(scaled, errors, group_scale)
    return (
        scaled.reshape(1, local_rows, width),
        errors.reshape(1, local_rows, width // OCT),
        group_scale,
        mean,
        total.reshape(()),
    )


def solution(mesh):
    placed = (P("expert", "row", None), P("expert", "row"), P("expert", None), P("expert", None))
    return jax.shard_map(
        body,
        mesh=mesh,
        in_specs=placed,
        out_specs=(
            P("expert", "row", None),
            P("expert", "row", None),
            P("expert", None),
            P("expert"),
            P(),
        ),
        check_vma=False,
    )
```
